32 devices in a mesh: seq: 8 (over z, x), img: 2 (over y), fsdp: 2 (over core).
Axes of the slice: x: 2, y: 2, z: 4, core: 2. Of those that a mesh axis runs over, the one named last changes fastest.
Arguments:
- vision_feats: bfloat16 [2, 2304, 1024], P('img', ('seq', 'fsdp')), may hold values from -6 to 6
- ln_gain: float32 [1024], replicated, may hold values from 0.5 to 1.5
- ln_bias: float32 [1024], replicated, may hold values from -3 to 3
- w_in: bfloat16 [1024, 4096], P('fsdp', 'seq'), may hold values from -0.1875 to 0.1875
- b_in: float32 [4096], P('seq'), may hold values from -3 to 3
- w_out: bfloat16 [4096, 4096], P('seq', 'fsdp'), may hold values from -0.09375 to 0.09375
- lm_grad: bfloat16 [2, 4096, 4096], P('img', 'seq', 'fsdp'), may hold values from -0.079589844 to 0.079589844
- image_counts: int32 [2, 2], P('img'), may hold values from 1 to 3, as said below
- token_pos: int32 [2, 2304], P('img'), may hold values from 0 to 2047, as said below
Outputs:
- w_in_grad: float32 [1024, 4096], P(('img', 'fsdp'), 'seq')
- b_in_grad: float32 [4096], replicated
- w_out_grad: float32 [4096, 4096], P(('seq', 'img'), 'fsdp')
- b_out_grad: float32 [4096], replicated
- ln_gain_grad: float32 [1024], replicated
- ln_bias_grad: float32 [1024], replicated
The draws below stay inside these ranges and needn't reach their ends.
Inputs may be any that keep to these rules, and one draw needn't show every extreme that they name: `image_counts`: in each group the 2 samples hold 4 images together, each sample one or more. `token_pos`: each image's 576 tokens take consecutive positions of its sample's sequence in order; a sample's images come in order without intersection, and images are numbered sample by sample as image_counts gives.
All inputs are finite; a program needn't handle non-finite values.
Results may differ from the reference program's by a relative error of at most 0.0047.
Values may be sent and summed in bfloat16 or wider, within the bound.
A program may use at most 128 MiB of HBM per device.

```python
import jax
import jax.numpy as jnp
from jax import lax

D = 4096
DV = 1024
HID = 4096
PATCH = 576
IMGS = 4
LEN = 2048
IMG_ROWS = 2304
POS = 4096
GROUPS = 2


def image_layout(key):
    base_key = jax.random.fold_in(key, 311)
    count_key, place_key = jax.random.split(base_key)
    first_count = 1 + jax.random.randint(count_key, (GROUPS,), 0, 3)
    counts = jnp.stack([first_count, IMGS - first_count], axis=1).astype(jnp.int32)
    text_room = LEN - counts * PATCH
    marks = jax.random.randint(place_key, (GROUPS, 2, 3), 0, 1 + text_room[:, :, None])
    marks = jnp.sort(marks, axis=2).astype(jnp.int32)
    pieces = []
    for image_index in range(IMGS):
        in_second = image_index >= first_count
        sample = in_second.astype(jnp.int32)
        slot_index = jnp.where(in_second, image_index - first_count, image_index).astype(jnp.int32)
        mark_row = jnp.take_along_axis(marks, sample[:, None, None], axis=1)[:, 0, :]
        begin_pos = jnp.take_along_axis(mark_row, slot_index[:, None], axis=1)[:, 0] + slot_index * PATCH
        pieces.append(begin_pos[:, None] + jnp.arange(PATCH, dtype=jnp.int32)[None, :])
    positions = jnp.concatenate(pieces, axis=1).astype(jnp.int32)
    return (counts, positions)


def draw_image_counts(key, part):
    counts, positions = image_layout(key)
    return counts


def draw_token_pos(key, part):
    counts, positions = image_layout(key)
    return positions


def shard_levels(key, shape, cuts, low, top_value):
    def one(position, parts):
        draws = jax.random.uniform(jax.random.fold_in(jax.random.fold_in(key, 6), position), (parts,), jnp.float32, low / len(cuts), top_value / len(cuts))
        return jnp.repeat(jnp.exp(draws), shape[position] // parts).reshape((-1,) + (1,) * (len(shape) - position - 1))

    loudness = one(*cuts[0])
    for cut in cuts[1:]:
        loudness = loudness * one(*cut)
    return loudness


def normal_values(stream_key, extent, deviation, limit, cuts=(), held_as=jnp.bfloat16):
    entries = jax.random.normal(stream_key, extent, jnp.float32) * deviation
    if len(cuts) > 0:
        entries = shard_levels(stream_key, extent, cuts, -0.22, 0.18) * entries
    return jnp.clip(entries, min=-limit, max=limit).astype(held_as)


def setup_inputs(seed: int = 0) -> dict:
    arg_keys = jax.random.split(jax.random.key(seed), 10)
    return {
        "vision_feats": normal_values(arg_keys[0], (GROUPS, IMG_ROWS, DV), 1.0, 6.0, ((0, 2), (1, 16))),
        "ln_gain": jnp.clip(1.0 + 0.1 * jax.random.normal(arg_keys[1], (DV,), jnp.float32), 0.5, 1.5),
        "ln_bias": normal_values(arg_keys[2], (DV,), 0.5, 3.0, (), jnp.float32),
        "w_in": normal_values(arg_keys[3], (DV, HID), DV ** -0.5, 0.1875, ((0, 2), (1, 8))),
        "b_in": normal_values(arg_keys[4], (HID,), 0.5, 3.0, ((0, 8),), jnp.float32),
        "w_out": normal_values(arg_keys[5], (HID, D), HID ** -0.5, 0.09375, ((0, 8), (1, 2))),
        "lm_grad": normal_values(arg_keys[6], (GROUPS, POS, D), 0.01, 0.079589844, ((0, 2), (1, 8), (2, 2))),
        "image_counts": draw_image_counts(jax.random.fold_in(arg_keys[9], 71), 0),
        "token_pos": draw_token_pos(jax.random.fold_in(arg_keys[9], 71), 0),
    }


def gelu_parts(preact):
    cumul = 0.5 * (1.0 + lax.erf(preact * 0.7071067811865476))
    density = jnp.exp(-0.5 * preact * preact) * 0.3989422804014327
    return (preact * cumul, cumul + preact * density)

def layer_norm(features, ln_gain, ln_bias):
    values = features.astype(jnp.float32)
    row_mean = lax.optimization_barrier(jnp.mean(values, axis=1, keepdims=True))
    centred = values - row_mean
    row_var = lax.optimization_barrier(jnp.mean(centred * centred, axis=1, keepdims=True))
    normed = centred * lax.rsqrt(row_var + 1e-05)
    return (normed, (normed * ln_gain + ln_bias).astype(jnp.bfloat16))

def absolute_positions(counts, positions):
    row_count = positions.shape[0]
    image_index = jnp.arange(row_count, dtype=jnp.int32) // PATCH
    bounds = jnp.cumsum(counts).astype(jnp.int32)
    sample = lax.optimization_barrier(jnp.sum((image_index[:, None] >= bounds[None, :]).astype(jnp.int32), axis=1))
    return (sample * LEN + positions).astype(jnp.int32)

def contract(left, right, left_dim, right_dim):
    return lax.dot_general(left, right, (((left_dim,), (right_dim,)), ((), ())), preferred_element_type=jnp.float32)

def reference(vision_feats, ln_gain, ln_bias, w_in, b_in, w_out, lm_grad, image_counts, token_pos):

    def one_group(totals, inputs):
        features, cotangent, counts, positions = inputs
        normed, normed_in = layer_norm(features, ln_gain, ln_bias)
        preact = jnp.dot(normed_in, w_in, preferred_element_type=jnp.float32) + b_in
        activ, slope = gelu_parts(preact)
        hidden = activ.astype(jnp.bfloat16)
        picked = cotangent[absolute_positions(counts, positions)]
        hidden_grad = contract(picked, w_out, 1, 1)
        preact_grad = (hidden_grad * slope).astype(jnp.bfloat16)
        normed_grad = contract(preact_grad, w_in, 1, 1)
        terms = (contract(normed_in, preact_grad, 0, 0), lax.optimization_barrier(jnp.sum(preact_grad, axis=0, dtype=jnp.float32)), contract(hidden, picked, 0, 0), lax.optimization_barrier(jnp.sum(picked, axis=0, dtype=jnp.float32)), lax.optimization_barrier(jnp.sum(normed_grad * normed, axis=0)), lax.optimization_barrier(jnp.sum(normed_grad, axis=0)))
        return (tuple((left + right for left, right in zip(totals, terms))), None)
    start_state = (jnp.zeros((DV, HID), jnp.float32), jnp.zeros((HID,), jnp.float32), jnp.zeros((HID, D), jnp.float32), jnp.zeros((D,), jnp.float32), jnp.zeros((DV,), jnp.float32), jnp.zeros((DV,), jnp.float32))
    totals, unused = lax.scan(one_group, start_state, (vision_feats, lm_grad, image_counts, token_pos))
    return (totals[0], totals[1], totals[2], totals[3], totals[4], totals[5])
```

```python
import functools

import jax
import jax.numpy as jnp
from jax import lax
from jax.experimental import pallas as pl
from jax.experimental.pallas import tpu as pltpu
from jax.sharding import PartitionSpec as P

PATCH = 576
CHUNKS = 2
PIECES = 8
EARLY = 3
BF16 = jnp.bfloat16
F32 = jnp.float32


def gelu_parts(preact):
    cumul = 0.5 * (1.0 + lax.erf(preact * 0.7071067811865476))
    density = jnp.exp(-0.5 * preact * preact) * 0.3989422804014327
    return (preact * cumul, cumul + preact * density)


def contract(left, right, left_dim, right_dim):
    return lax.dot_general(
        left, right, (((left_dim,), (right_dim,)), ((), ())), preferred_element_type=jnp.float32
    )


def shift(value, axis, amount):
    count = lax.axis_size(axis)
    return lax.ppermute(value, axis, [(i, (i + amount) % count) for i in range(count)])


def flip(value, bit):
    count = lax.axis_size("seq")
    return lax.ppermute(value, "seq", [(i, i ^ bit) for i in range(count)])


def pick(value, index, axis):
    return lax.dynamic_index_in_dim(value, index, axis=axis, keepdims=False)


def scatter_sum(value, axis):
    count = lax.axis_size(axis)
    index = lax.axis_index(axis)
    if count > 2:
        return lax.psum_scatter(value, axis, scatter_dimension=0, tiled=False)
    if count == 1:
        return value[0]
    sent = pick(value, 1 - index, 0).astype(jnp.bfloat16)
    return pick(value, index, 0) + shift(sent, axis, 1).astype(jnp.float32)


def sample_sum(value, stride, after):
    total, _ = lax.optimization_barrier((value[0], after))
    for k in range(1, value.shape[0]):
        moved = shift(value[k].astype(jnp.bfloat16), "seq", -k * stride)
        total = total + moved.astype(jnp.float32)
    return total


def per_device(vision_feats, ln_gain, ln_bias, w_in, b_in, w_out, lm_grad, image_counts, token_pos):
    seq_count = lax.axis_size("seq")
    seq_index = lax.axis_index("seq")
    img_count = lax.axis_size("img")
    fsdp_count = lax.axis_size("fsdp")
    fsdp_index = lax.axis_index("fsdp")
    lm_block = lm_grad[0]
    block_rows, half_width = lm_block.shape
    counts = image_counts[0]
    samples = counts.shape[0]
    stride = seq_count // samples
    sample_len = stride * block_rows
    own_sample = seq_index // stride
    positions = token_pos[0]
    row_count = positions.shape[0]
    images = row_count // PATCH
    starts = positions.reshape(images, PATCH)[:, 0]
    bounds = jnp.cumsum(counts)
    image_index = jnp.arange(images, dtype=jnp.int32)
    image_sample = jnp.sum((image_index[:, None] >= bounds[None, :]).astype(jnp.int32), axis=1)
    in_sample = image_sample == own_sample

    def lookup(place):
        offset = place[:, None] - starts[None, :]
        match = in_sample[None, :] & (offset >= 0) & (offset < PATCH)
        row = jnp.sum(jnp.where(match, offset + image_index[None, :] * PATCH, 0), axis=1)
        return row, jnp.any(match, axis=1)

    own_place = (seq_index % stride) * block_rows + jnp.arange(block_rows, dtype=jnp.int32)
    own_mask = lookup(own_place)[1].astype(jnp.bfloat16)
    out_bias_half = jnp.dot(own_mask[None, :], lm_block, preferred_element_type=jnp.float32)[0]
    out_bias_whole = lax.dynamic_update_slice_in_dim(
        jnp.zeros((half_width * fsdp_count,), jnp.float32),
        out_bias_half,
        fsdp_index * half_width,
        0,
    )

    feats = lax.all_gather(vision_feats[0], ("seq", "fsdp"), axis=0, tiled=True)

    in_blocks = [w_in] + [shift(w_in, "seq", k * stride) for k in range(1, samples)]
    in_bias = jnp.concatenate([b_in] + [shift(b_in, "seq", k * stride) for k in range(1, samples)])
    w_in_half = jnp.concatenate(in_blocks, axis=1)
    w_in_full = lax.all_gather(w_in_half, "fsdp", axis=0, tiled=True)
    w_out_later, _ = lax.optimization_barrier((w_out, w_in_half))
    w_out_full = jnp.concatenate(
        [w_out] + [shift(w_out_later, "seq", k * stride) for k in range(1, samples)], axis=0
    )
    hid = in_bias.shape[0]
    block_hid = hid // samples

    groups = [[s * stride + i for i in range(stride)] for s in range(samples)]
    width = half_width // CHUNKS
    slices = [lm_block[:, c * width : (c + 1) * width] for c in range(CHUNKS)]
    crossed = stride == 4
    if crossed:
        pieces = []
        for piece in slices:
            far = flip(piece, 2)
            near = flip(piece, 1)
            pieces.append(jnp.concatenate([piece, near, far, flip(far, 1)], axis=0))
    else:
        pieces = [
            lax.all_gather(piece, "seq", axis=0, tiled=True, axis_index_groups=groups)
            for piece in slices
        ]
    b_out_grad = lax.psum(out_bias_whole, ("seq", "img", "fsdp"))
    feats, b_out_grad = lax.optimization_barrier((feats, b_out_grad))

    part_len = sample_len // fsdp_count
    place = fsdp_index * part_len + jnp.arange(part_len, dtype=jnp.int32)
    if crossed:
        block = place // block_rows
        place = (block ^ (seq_index % stride)) * block_rows + place % block_rows
    row, mask = lookup(place)
    values = feats.at[row].get(mode="promise_in_bounds").astype(jnp.float32)
    row_mean = jnp.mean(values, axis=1, keepdims=True)
    centred = values - row_mean
    row_var = jnp.mean(centred * centred, axis=1, keepdims=True)
    normed = centred * lax.rsqrt(row_var + 1e-05)
    normed_in = (normed * ln_gain + ln_bias).astype(jnp.bfloat16)
    preact = jnp.dot(normed_in, w_in_full, preferred_element_type=jnp.float32) + in_bias
    activ, slope = gelu_parts(preact)
    hidden = jnp.where(mask[:, None], activ, 0.0).astype(jnp.bfloat16)
    slope = jnp.where(mask[:, None], slope, 0.0)
    if fsdp_count == 2:
        other = shift(hidden, "fsdp", 1)
        first = fsdp_index == 0
        hidden_full = jnp.concatenate(
            [jnp.where(first, hidden, other), jnp.where(first, other, hidden)], axis=0
        )
    else:
        hidden_full = lax.all_gather(hidden, "fsdp", axis=0, tiled=True)

    w_out_grads = []
    hidden_part = 0.0
    hidden_full, pieces[0] = lax.optimization_barrier((hidden_full, pieces[0]))
    for c in range(CHUNKS):
        piece = pieces[c]
        part = contract(hidden_full, piece, 0, 0)
        part = part.reshape(samples, img_count, block_hid // img_count, width)
        part = scatter_sum(part.transpose(1, 0, 2, 3), "img")
        w_out_grads.append(part)
        hidden_part = hidden_part + contract(
            piece, w_out_full[:, c * width : (c + 1) * width], 1, 1
        )

    hidden_grad = scatter_sum(hidden_part.reshape(fsdp_count, part_len, hid), "fsdp")
    preact_grad = (hidden_grad * slope).astype(jnp.bfloat16)
    in_part = contract(normed_in, preact_grad, 0, 0)
    in_part = in_part.reshape(img_count, fsdp_count, -1, samples, block_hid)
    in_part = scatter_sum(in_part.transpose(1, 0, 2, 3, 4), "fsdp")
    in_part = scatter_sum(in_part, "img")

    b_in_part = jnp.sum(preact_grad, axis=0, dtype=jnp.float32)
    normed_grad = contract(preact_grad, w_in_full, 1, 1)
    gain_part = jnp.sum(normed_grad * normed, axis=0)
    bias_part = jnp.sum(normed_grad, axis=0)
    hidden_bias = jnp.zeros((seq_count, block_hid), jnp.float32)
    for k in range(samples):
        owner = (seq_index - k * stride + seq_count) % seq_count
        hidden_bias = lax.dynamic_update_slice(
            hidden_bias, b_in_part[None, k * block_hid : (k + 1) * block_hid], (owner, 0)
        )
    gain_grad, bias_grad, b_in_grad = lax.psum(
        (gain_part, bias_part, hidden_bias.reshape(-1)), ("seq", "img", "fsdp")
    )
    w_in_grad = sample_sum(in_part.transpose(1, 0, 2), stride, gain_grad)
    w_out_grad = jnp.concatenate(
        [sample_sum(part, stride, gain_grad) for part in w_out_grads], axis=1
    )
    return (w_in_grad, b_in_grad, w_out_grad, b_out_grad, gain_grad, bias_grad)


def kernel_body(
    dims,
    counts_ref,
    pos_ref,
    feats_ref,
    gain_ref,
    bias_ref,
    wi_ref,
    bin_ref,
    wo_ref,
    lm_ref,
    wo_out,
    wi_out,
    small_out,
    L,
    W,
    WI,
    F,
    NT,
    V,
    MEAN,
    RSTD,
    SL,
    HT,
    HP,
    PG,
    HR,
    YS,
    YR,
    ZS,
    ZR,
    GP,
    WS,
    WR,
    WYS,
    WYR,
    WZS,
    WZR,
    PB,
    ACC,
    SV,
    AR,
    send_sem,
    recv_sem,
    local_sem,
):
    rows, half, hb, dv, frows, tokens, seq_count, samples, images = dims
    stride = seq_count // samples
    span = stride * rows
    part = span // 2
    hid = samples * hb
    hh = hb // 2
    dvh = dv // 2
    dvq = dv // 4
    ck = half // PIECES
    seq = lax.axis_index("seq")
    img = lax.axis_index("img")
    core = lax.axis_index("fsdp")

    def flip(value, bits):
        for bit in (1, 2, 4):
            if bits & bit:
                value = value + bit - 2 * bit * ((value // bit) % 2)
        return value

    def device(bits=0, y=0, c=0):
        return (
            flip(seq, bits),
            1 - img if y else img,
            1 - core if c else core,
        )

    z1 = device(2)
    z2 = device(4)
    z3 = device(6)
    xn = device(1)
    yn = device(y=1)
    sib = device(c=1)

    names = {}

    def slot(name, count=1):
        if name not in names:
            names[name] = sum(c for _, c in names.values()), count
        return names[name][0]

    def remote(src, dst, target, recv, send=None, k=0, count=1):
        return pltpu.make_async_remote_copy(
            src_ref=src,
            dst_ref=dst,
            send_sem=send_sem.at[slot(send or recv, count) + k],
            recv_sem=recv_sem.at[slot(recv, count) + k],
            device_id=target,
            device_id_type=pl.DeviceIdType.MESH,
        )

    started = []

    def start(*args, **kwargs):
        copy = remote(*args, **kwargs)
        copy.start()
        started.append(copy)

    def aligned(value, unit):
        return pl.multiple_of(value, unit)

    def feat_block(bits, c):
        return F.at[pl.ds(aligned((flip(seq, bits) * 2 + c) * frows, 16), frows)]

    barrier = pltpu.get_barrier_semaphore()
    for target in (z1, z2, z3, xn, yn, sib):
        pl.semaphore_signal(
            barrier, inc=1, device_id=target, device_id_type=pl.DeviceIdType.MESH
        )

    locals_ = [
        pltpu.make_async_copy(feats_ref, feat_block(0, core), local_sem.at[0]),
        pltpu.make_async_copy(
            wi_ref, WI.at[0, pl.ds(aligned(core * dvh, dvh), dvh)], local_sem.at[1]
        ),
        pltpu.make_async_copy(lm_ref, L.at[pl.ds(0, rows)], local_sem.at[2]),
        pltpu.make_async_copy(wo_ref, W.at[0], local_sem.at[3]),
    ]
    for copy in locals_:
        copy.start()
    pl.semaphore_wait(barrier, 6)

    def lm_piece(k, index):
        columns = pl.ds(aligned(k * ck, ck), ck)
        return L.at[pl.ds(index * rows, rows), columns]

    def lm_own(k):
        return lm_ref.at[:, pl.ds(aligned(k * ck, ck), ck)]

    def x_copy(k):
        return remote(lm_own(k), lm_piece(k, 1), xn, "X", k=k, count=PIECES)

    def z_copy(k):
        return remote(lm_own(k), lm_piece(k, 2), z1, "Z", k=k, count=PIECES)

    def d_copy(k):
        return remote(lm_piece(k, 2), lm_piece(k, 3), xn, "D", k=k, count=PIECES)

    zseq = seq // 2
    inner = (zseq + 1) // 2 == 1
    wi_rows = pl.ds(aligned(img * dvq, dvq), dvq)
    wi_mine = WI.at[1, pl.ds(aligned(core * dvh + img * dvq, dvq), dvq)]
    wi_other = WI.at[1, pl.ds(aligned(core * dvh + (1 - img) * dvq, dvq), dvq)]
    wo_mine = pl.ds(aligned(img * hh, hh), hh)

    start(feats_ref, feat_block(0, core), z1, "F2")
    start(wi_ref.at[wi_rows], wi_mine, z2, "WIZ")
    start(bin_ref, PB, z2, "BZ")
    for k in range(EARLY):
        z_copy(k).start()
    start(feats_ref, feat_block(0, core), xn, "F1")
    for k in range(EARLY):
        x_copy(k).start()
    start(feats_ref, feat_block(0, core), sib, "S0")
    start(wi_ref, WI.at[0, pl.ds(aligned(core * dvh, dvh), dvh)], sib, "WIS0")

    def arrive(bits, name):
        remote(feats_ref, feat_block(bits, core), xn, name).wait_recv()

    def hand_x(bits):
        block = feat_block(bits, core)
        start(block, block, xn, f"F{bits + 1}")

    def hand_sib(bits):
        block = feat_block(bits, core)
        start(block, block, sib, f"S{bits}")

    arrive(2, "F2")
    locals_[0].wait()
    own_block, pair_block = feat_block(0, core), feat_block(2, core)
    far_block, near_block = feat_block(4, core), feat_block(6, core)
    cut_own = remote(own_block, own_block, z3, "F6", send="C0")
    cut_pair = remote(pair_block, pair_block, z3, "F4", send="C1")
    back_near = remote(near_block, near_block, z1, "F4", send="C2")
    back_far = remote(far_block, far_block, z1, "F6", send="C3")

    @pl.when(inner)
    def _():
        cut_own.start()
        cut_pair.start()

    hand_x(2)
    hand_sib(2)
    start(wo_ref.at[wo_mine], W.at[1, wo_mine], z2, "WZ")
    arrive(4, "F4")
    arrive(6, "F6")

    @pl.when(inner)
    def _():
        back_near.start()
        back_far.start()

    for bits in (4, 6):
        hand_x(bits)
        hand_sib(bits)

    @pl.loop(EARLY, PIECES)
    def _(k):
        z_copy(k).start()
        x_copy(k).start()

    remote(wi_ref.at[wi_rows], wi_mine, z2, "WIZ").wait_recv()
    start(wi_mine, wi_mine, yn, "WIY")
    start(wi_mine, wi_mine, sib, "WIS1")
    for bits in (1, 3, 5, 7):
        arrive(bits, f"F{bits}")
        hand_sib(bits)
    remote(wi_other, wi_other, yn, "WIY").wait_recv()
    start(wi_other, wi_other, sib, "WIS2")
    for k in range(EARLY):
        z_copy(k).wait_recv()
        d_copy(k).start()
    remote(bin_ref, PB, z2, "BZ").wait_recv()
    remote(
        wi_ref, WI.at[0, pl.ds(aligned((1 - core) * dvh, dvh), dvh)], sib, "WIS0"
    ).wait_recv()
    for name, y in (("WIS1", img), ("WIS2", 1 - img)):
        piece = WI.at[1, pl.ds(aligned((1 - core) * dvh + y * dvq, dvq), dvq)]
        remote(piece, piece, sib, name).wait_recv()
    for bits in range(8):
        block = feat_block(bits, 1 - core)
        remote(block, block, sib, f"S{bits}").wait_recv()
    for copy in locals_[1:]:
        copy.wait()

    inside = seq % stride
    sample = seq // stride
    bounds = [counts_ref[0, 0] * 0]
    for s in range(samples):
        bounds.append(bounds[-1] + counts_ref[0, s])
    low = bounds[0]
    high = bounds[1]
    for s in range(1, samples):
        low = jnp.where(sample == s, bounds[s], low)
        high = jnp.where(sample == s, bounds[s + 1], high)
    begins = []
    for n in range(images):
        here = jnp.where(n >= low, jnp.where(n < high, 1, 0), 0)
        begins.append(jnp.where(here == 1, pos_ref[0, n * PATCH], 2 * span))

    def lookup(place):
        row = jnp.full(place.shape, -1, jnp.int32)
        for n in range(images):
            offset = place - begins[n]
            match = jnp.logical_and(offset >= 0, offset < PATCH)
            row = jnp.where(match, offset + n * PATCH, row)
        return row

    def place_of(index, count, first):
        base = flip(inside, 0) * 0
        return base + first + lax.broadcasted_iota(jnp.int32, (count, 1), 0)

    tile = 256
    per_slot = rows // tile

    @pl.loop(0, part // tile)
    def _(t):
        low_bit = (t // per_slot) % 2
        block = inside + low_bit - 2 * low_bit * (inside % 2)
        block = block + 2 * core - 4 * core * ((block // 2) % 2)
        first = block * rows + (t % per_slot) * tile
        place = first + lax.broadcasted_iota(jnp.int32, (tile, 1), 0)
        row = lookup(place)
        kept = jnp.where(row >= 0, 1.0, 0.0).astype(F32)
        wanted = lax.broadcasted_iota(jnp.int32, (tile, tokens), 1) == row
        chosen = jnp.where(wanted, 1.0, 0.0).astype(BF16)
        values = jnp.dot(chosen, F[...], preferred_element_type=F32)
        here = pl.ds(aligned(t * tile, tile), tile)
        V[here] = values.astype(BF16)
        mean = jnp.mean(values, axis=1, keepdims=True)
        centred = values - mean
        rstd = lax.rsqrt(jnp.mean(centred * centred, axis=1, keepdims=True) + 1e-05)
        MEAN[here] = mean
        RSTD[here] = rstd
        scaled = centred * rstd * gain_ref[...] + bias_ref[...]
        normed_in = scaled.astype(BF16)
        NT[:, here] = scaled.T.astype(BF16)
        for g in range(samples):
            shift_row = bin_ref[...] if g == 0 else PB[...]
            preact = jnp.dot(normed_in, WI[g], preferred_element_type=F32) + shift_row
            activ, slope = gelu_parts(preact)
            columns = pl.ds(g * hb, hb)
            SL[here, columns] = slope * kept
            HT[columns, pl.ds(aligned(core * part + t * tile, tile), tile)] = (
                (activ * kept).T.astype(BF16)
            )

    ht_mine = HT.at[:, pl.ds(aligned(core * part, part), part)]
    ht_other = HT.at[:, pl.ds(aligned((1 - core) * part, part), part)]
    start(ht_mine, ht_mine, sib, "HT")

    place = inside * rows + lax.broadcasted_iota(jnp.int32, (rows, 1), 0)
    own_kept = jnp.where(lookup(place) >= 0, 1.0, 0.0).astype(F32)
    SV[0] = jnp.zeros(SV.shape[1:], F32)
    pieces = dv // hb
    out_row = 2 * pieces + seq_count
    for m in range(half // hb):
        block = L[pl.ds(0, rows), pl.ds(m * hb, hb)].astype(F32) * own_kept
        total = jnp.sum(block, axis=0, keepdims=True)
        SV[0, pl.ds(out_row + core * (half // hb) + m, 1)] = total

    remote(wo_ref.at[wo_mine], W.at[1, wo_mine], z2, "WZ").wait_recv()
    start(W.at[1, wo_mine], W.at[1, wo_mine], yn, "WY")
    remote(ht_other, ht_other, sib, "HT").wait_recv()

    HP[...] = jnp.zeros(HP.shape, F32)

    def y_copy(k):
        columns = pl.ds(aligned(k * ck, ck), ck)
        return remote(YS.at[:, columns], YR.at[:, columns], yn, "YK", k=k, count=PIECES)

    def zk_copy(k):
        columns = pl.ds(aligned(k * ck, ck), ck)
        return remote(ZS.at[:, columns], ZR.at[:, columns], z2, "ZK", k=k, count=PIECES)

    def weight_grad(k):
        columns = pl.ds(aligned(k * ck, ck), ck)
        piece = L[:, columns]
        for g in range(samples):
            mine = pl.ds(aligned(g * hb + img * hh, hh), hh)
            other = pl.ds(aligned(g * hb + (1 - img) * hh, hh), hh)
            sent = jnp.dot(HT[other], piece, preferred_element_type=F32)
            YS[pl.ds(g * hh, hh), columns] = sent.astype(BF16)
            kept = jnp.dot(HT[mine], piece, preferred_element_type=F32)
            if g == 0:
                wo_out[:, columns] = kept
            else:
                GP[:, columns] = kept
        y_copy(k).start()

    def hidden_part(k, g):
        columns = pl.ds(aligned(k * ck, ck), ck)

        @pl.loop(0, 2 * part // rows)
        def _(t):
            per = part // rows
            here = pl.ds(aligned((t % per) * rows, rows), rows)
            HP[t // per, here, pl.ds(g * hb, hb)] += lax.dot_general(
                L[pl.ds(aligned(t * rows, rows), rows), columns],
                W[g, :, columns],
                (((1,), (1,)), ((), ())),
                preferred_element_type=F32,
            )

    def over_img(k):
        columns = pl.ds(aligned(k * ck, ck), ck)
        y_copy(k).wait_recv()
        wo_out[:, columns] += YR[pl.ds(0, hh), columns].astype(F32)
        both = GP[:, columns] + YR[pl.ds(hh, hh), columns].astype(F32)
        ZS[:, columns] = both.astype(BF16)
        zk_copy(k).start()

    def over_samples(k):
        columns = pl.ds(aligned(k * ck, ck), ck)
        zk_copy(k).wait_recv()
        wo_out[:, columns] += ZR[:, columns].astype(F32)

    @pl.loop(0, PIECES)
    def _(k):
        @pl.when(k + EARLY < PIECES)
        def _():
            z_copy(k + EARLY).wait_recv()
            d_copy(k + EARLY).start()

        x_copy(k).wait_recv()
        d_copy(k).wait_recv()
        weight_grad(k)
        hidden_part(k, 0)

        @pl.when(k >= 1)
        def _():
            over_img(k - 1)

        @pl.when(k >= 2)
        def _():
            over_samples(k - 2)

        @pl.when(k == PIECES // 2)
        def _():
            wo_other = pl.ds(aligned((1 - img) * hh, hh), hh)
            remote(W.at[1, wo_other], W.at[1, wo_other], yn, "WY").wait_recv()

        @pl.when(k >= PIECES // 2)
        def _():
            for g in range(1, samples):
                hidden_part(2 * k - PIECES, g)
                hidden_part(2 * k + 1 - PIECES, g)

    @pl.loop(0, part // tile)
    def _(t):
        here = pl.ds(aligned(t * tile, tile), tile)
        PG[here] = HP[1 - core, here].astype(BF16)

    half_sum = remote(PG, HR, sib, "HR")
    half_sum.start()
    over_img(PIECES - 1)
    over_samples(PIECES - 2)
    half_sum.wait()

    ACC[...] = jnp.zeros(ACC.shape, F32)

    @pl.loop(0, part // tile)
    def _(t):
        here = pl.ds(aligned(t * tile, tile), tile)
        grad = HP[core, here] + HR[here].astype(F32)
        rounded = (grad * SL[here]).astype(BF16)
        PG[here] = rounded
        ACC[pl.ds(0, 1)] += jnp.sum(rounded.astype(F32), axis=0, keepdims=True)

    def first_grad(block):
        lines = pl.ds(aligned(block * dvq, dvq), dvq)
        return jnp.dot(NT[lines], PG[...], preferred_element_type=F32)

    for y in range(2):
        WS[y] = first_grad(2 * y + 1 - core).astype(BF16)
    start(WS, WR, sib, "WG")
    kept_rows = [pl.ds(y * dvq, dvq) for y in range(2)]
    for y in range(2):
        HP[1 - core, kept_rows[y]] = first_grad(2 * y + core)
    remote(WS, WR, sib, "WG").wait_recv()
    other_rows = pl.ds(aligned((1 - img) * dvq, dvq), dvq)
    mine_rows = pl.ds(aligned(img * dvq, dvq), dvq)
    WYS[...] = (HP[1 - core, other_rows] + WR[1 - img].astype(F32)).astype(BF16)
    own_cols, far_cols = pl.ds(0, hb), pl.ds(hb, hb)
    start(WYS.at[:, far_cols], WYR.at[:, far_cols], yn, "WYF")
    start(WYS.at[:, own_cols], WYR.at[:, own_cols], yn, "WYO")

    @pl.loop(0, part // tile)
    def _(t):
        here = pl.ds(aligned(t * tile, tile), tile)
        grad = jnp.zeros((tile, dv), F32)
        for g in range(samples):
            grad = grad + lax.dot_general(
                PG[here, pl.ds(g * hb, hb)],
                WI[g],
                (((1,), (1,)), ((), ())),
                preferred_element_type=F32,
            )
        normed = (V[here].astype(F32) - MEAN[here]) * RSTD[here]
        ACC[pl.ds(1, 1)] += jnp.sum(grad * normed, axis=0, keepdims=True)
        ACC[pl.ds(2, 1)] += jnp.sum(grad, axis=0, keepdims=True)

    for m in range(pieces):
        columns = pl.ds(m * hb, hb)
        SV[0, pl.ds(m, 1)] = ACC[pl.ds(1, 1), columns]
        SV[0, pl.ds(pieces + m, 1)] = ACC[pl.ds(2, 1), columns]
    for g in range(samples):
        line = 2 * pieces + flip(seq, 4 * g)
        SV[0, pl.ds(line, 1)] = ACC[pl.ds(0, 1), pl.ds(g * hb, hb)]

    def small_start(n, target):
        start(SV.at[n], AR.at[n], target, f"AR{n}")

    def small_end(n):
        remote(SV.at[n], AR.at[n], sib, f"AR{n}").wait_recv()
        return SV[n] + AR[n]

    small_start(0, sib)
    remote(WYS.at[:, far_cols], WYR.at[:, far_cols], yn, "WYF").wait_recv()
    WZS[...] = (HP[1 - core, mine_rows, far_cols] + WR[img, :, far_cols].astype(F32)
                + WYR[:, far_cols].astype(F32)).astype(BF16)
    start(WZS, WZR, z2, "WZS")
    SV[1] = small_end(0)
    small_start(1, xn)
    over_samples(PIECES - 1)
    SV[2] = small_end(1)
    small_start(2, yn)
    remote(WYS.at[:, own_cols], WYR.at[:, own_cols], yn, "WYO").wait_recv()
    wi_out[...] = (HP[1 - core, mine_rows, own_cols] + WR[img, :, own_cols].astype(F32)
                   + WYR[:, own_cols].astype(F32))
    SV[3] = small_end(2)
    small_start(3, z1)
    SV[4] = small_end(3)
    small_start(4, z2)
    remote(WZS, WZR, z2, "WZS").wait_recv()
    wi_out[...] += WZR[...].astype(F32)
    small_out[...] = small_end(4)

    for copy in started:
        copy.wait_send()

    @pl.when(inner)
    def _():
        for copy in (cut_own, cut_pair, back_near, back_far):
            copy.wait_send()

    @pl.loop(0, PIECES)
    def _(k):
        for copy in (x_copy, z_copy, d_copy, y_copy, zk_copy):
            copy(k).wait_send()


def per_device_kernel(
    vision_feats, ln_gain, ln_bias, w_in, b_in, w_out, lm_grad, image_counts, token_pos
):
    seq_count = lax.axis_size("seq")
    _, rows, half = lm_grad.shape
    hb = w_out.shape[0]
    dv = ln_gain.shape[0]
    frows = vision_feats.shape[1]
    tokens = token_pos.shape[1]
    samples = image_counts.shape[1]
    stride = seq_count // samples
    span = stride * rows
    part = span // 2
    hid = samples * hb
    images = tokens // PATCH
    small = 2 * (dv // hb) + seq_count + 2 * (half // hb)
    small = -(-small // 8) * 8
    dims = (rows, half, hb, dv, frows, tokens, seq_count, samples, images)
    vmem = pl.BlockSpec(memory_space=pltpu.VMEM)
    smem = pl.BlockSpec(memory_space=pltpu.SMEM)
    hbm = pl.BlockSpec(memory_space=pl.ANY)
    wo, wi, sums = pl.pallas_call(
        functools.partial(kernel_body, dims),
        out_shape=(
            jax.ShapeDtypeStruct((hb // 2, half), F32),
            jax.ShapeDtypeStruct((dv // 4, hb), F32),
            jax.ShapeDtypeStruct((small, hb), F32),
        ),
        in_specs=[smem, smem, hbm, vmem, vmem, hbm, vmem, hbm, hbm],
        out_specs=[vmem, vmem, vmem],
        scratch_shapes=[
            pltpu.VMEM((span, half), BF16),
            pltpu.VMEM((samples, hb, half), BF16),
            pltpu.VMEM((samples, dv, hb), BF16),
            pltpu.VMEM((tokens, dv), BF16),
            pltpu.VMEM((dv, part), BF16),
            pltpu.VMEM((part, dv), BF16),
            pltpu.VMEM((part, 1), F32),
            pltpu.VMEM((part, 1), F32),
            pltpu.VMEM((part, hid), F32),
            pltpu.VMEM((hid, span), BF16),
            pltpu.VMEM((2, part, hid), F32),
            pltpu.VMEM((part, hid), BF16),
            pltpu.VMEM((part, hid), BF16),
            pltpu.VMEM((hb, half), BF16),
            pltpu.VMEM((hb, half), BF16),
            pltpu.VMEM((hb // 2, half), BF16),
            pltpu.VMEM((hb // 2, half), BF16),
            pltpu.VMEM((hb // 2, half), F32),
            pltpu.VMEM((2, dv // 4, hid), BF16),
            pltpu.VMEM((2, dv // 4, hid), BF16),
            pltpu.VMEM((dv // 4, hid), BF16),
            pltpu.VMEM((dv // 4, hid), BF16),
            pltpu.VMEM((dv // 4, hb), BF16),
            pltpu.VMEM((dv // 4, hb), BF16),
            pltpu.VMEM((1, hb), F32),
            pltpu.VMEM((8, max(hid, dv)), F32),
            pltpu.VMEM((5, small, hb), F32),
            pltpu.VMEM((5, small, hb), F32),
            pltpu.SemaphoreType.DMA((96,)),
            pltpu.SemaphoreType.DMA((96,)),
            pltpu.SemaphoreType.DMA((4,)),
        ],
        compiler_params=pltpu.CompilerParams(
            collective_id=0, has_side_effects=True, vmem_limit_bytes=67043328
        ),
    )(
        image_counts,
        token_pos,
        vision_feats[0],
        ln_gain[None],
        ln_bias[None],
        w_in,
        b_in[None],
        w_out,
        lm_grad[0],
    )
    pieces = dv // hb
    at = (0, pieces, 2 * pieces, 2 * pieces + seq_count)
    gain_grad = sums[at[0] : at[1]].reshape(-1)
    bias_grad = sums[at[1] : at[2]].reshape(-1)
    b_in_grad = sums[at[2] : at[3]].reshape(-1)
    b_out_grad = sums[at[3] : at[3] + 2 * (half // hb)].reshape(-1)
    return (wi, b_in_grad, wo, b_out_grad, gain_grad, bias_grad)


def dispatch(mesh, *args):
    sizes = (mesh.shape["seq"], mesh.shape["img"], mesh.shape["fsdp"])
    if sizes == (8, 2, 2) and args[7].shape[1] == 2:
        return per_device_kernel(*args)
    return per_device(*args)


def solution(mesh):
    return jax.shard_map(
        functools.partial(dispatch, mesh),
        mesh=mesh,
        in_specs=(
            P("img", ("seq", "fsdp"), None),
            P(),
            P(),
            P("fsdp", "seq"),
            P("seq"),
            P("seq", "fsdp"),
            P("img", "seq", "fsdp"),
            P("img", None),
            P("img", None),
        ),
        out_specs=(
            P(("img", "fsdp"), "seq"),
            P(),
            P(("seq", "img"), "fsdp"),
            P(),
            P(),
            P(),
        ),
        check_vma=False,
    )
```

```python
import functools

import jax
import jax.numpy as jnp
from jax import lax
from jax.experimental import pallas as pl
from jax.experimental.pallas import tpu as pltpu
from jax.sharding import PartitionSpec as P

PATCH = 576
CHUNKS = 2
PIECES = 8
EARLY_X = 3
EARLY_Z = 2
AHEAD_X = 6
AHEAD_D = 3
LATE_MINE = 3
LATE = 5
BF16 = jnp.bfloat16
F32 = jnp.float32


def gelu_parts(preact):
    cumul = 0.5 * (1.0 + lax.erf(preact * 0.7071067811865476))
    density = jnp.exp(-0.5 * preact * preact) * 0.3989422804014327
    return (preact * cumul, cumul + preact * density)


def contract(left, right, left_dim, right_dim):
    return lax.dot_general(
        left, right, (((left_dim,), (right_dim,)), ((), ())), preferred_element_type=jnp.float32
    )


def shift(value, axis, amount):
    count = lax.axis_size(axis)
    return lax.ppermute(value, axis, [(i, (i + amount) % count) for i in range(count)])


def flip(value, bit):
    count = lax.axis_size("seq")
    return lax.ppermute(value, "seq", [(i, i ^ bit) for i in range(count)])


def pick(value, index, axis):
    return lax.dynamic_index_in_dim(value, index, axis=axis, keepdims=False)


def scatter_sum(value, axis):
    count = lax.axis_size(axis)
    index = lax.axis_index(axis)
    if count > 2:
        return lax.psum_scatter(value, axis, scatter_dimension=0, tiled=False)
    if count == 1:
        return value[0]
    sent = pick(value, 1 - index, 0).astype(jnp.bfloat16)
    return pick(value, index, 0) + shift(sent, axis, 1).astype(jnp.float32)


def sample_sum(value, stride, after):
    total, _ = lax.optimization_barrier((value[0], after))
    for k in range(1, value.shape[0]):
        moved = shift(value[k].astype(jnp.bfloat16), "seq", -k * stride)
        total = total + moved.astype(jnp.float32)
    return total


def per_device(vision_feats, ln_gain, ln_bias, w_in, b_in, w_out, lm_grad, image_counts, token_pos):
    seq_count = lax.axis_size("seq")
    seq_index = lax.axis_index("seq")
    img_count = lax.axis_size("img")
    fsdp_count = lax.axis_size("fsdp")
    fsdp_index = lax.axis_index("fsdp")
    lm_block = lm_grad[0]
    block_rows, half_width = lm_block.shape
    counts = image_counts[0]
    samples = counts.shape[0]
    stride = seq_count // samples
    sample_len = stride * block_rows
    own_sample = seq_index // stride
    positions = token_pos[0]
    row_count = positions.shape[0]
    images = row_count // PATCH
    starts = positions.reshape(images, PATCH)[:, 0]
    bounds = jnp.cumsum(counts)
    image_index = jnp.arange(images, dtype=jnp.int32)
    image_sample = jnp.sum((image_index[:, None] >= bounds[None, :]).astype(jnp.int32), axis=1)
    in_sample = image_sample == own_sample

    def lookup(place):
        offset = place[:, None] - starts[None, :]
        match = in_sample[None, :] & (offset >= 0) & (offset < PATCH)
        row = jnp.sum(jnp.where(match, offset + image_index[None, :] * PATCH, 0), axis=1)
        return row, jnp.any(match, axis=1)

    own_place = (seq_index % stride) * block_rows + jnp.arange(block_rows, dtype=jnp.int32)
    own_mask = lookup(own_place)[1].astype(jnp.bfloat16)
    out_bias_half = jnp.dot(own_mask[None, :], lm_block, preferred_element_type=jnp.float32)[0]
    out_bias_whole = lax.dynamic_update_slice_in_dim(
        jnp.zeros((half_width * fsdp_count,), jnp.float32),
        out_bias_half,
        fsdp_index * half_width,
        0,
    )

    feats = lax.all_gather(vision_feats[0], ("seq", "fsdp"), axis=0, tiled=True)

    in_blocks = [w_in] + [shift(w_in, "seq", k * stride) for k in range(1, samples)]
    in_bias = jnp.concatenate([b_in] + [shift(b_in, "seq", k * stride) for k in range(1, samples)])
    w_in_half = jnp.concatenate(in_blocks, axis=1)
    w_in_full = lax.all_gather(w_in_half, "fsdp", axis=0, tiled=True)
    w_out_later, _ = lax.optimization_barrier((w_out, w_in_half))
    w_out_full = jnp.concatenate(
        [w_out] + [shift(w_out_later, "seq", k * stride) for k in range(1, samples)], axis=0
    )
    hid = in_bias.shape[0]
    block_hid = hid // samples

    groups = [[s * stride + i for i in range(stride)] for s in range(samples)]
    width = half_width // CHUNKS
    slices = [lm_block[:, c * width : (c + 1) * width] for c in range(CHUNKS)]
    crossed = stride == 4
    if crossed:
        pieces = []
        for piece in slices:
            far = flip(piece, 2)
            near = flip(piece, 1)
            pieces.append(jnp.concatenate([piece, near, far, flip(far, 1)], axis=0))
    else:
        pieces = [
            lax.all_gather(piece, "seq", axis=0, tiled=True, axis_index_groups=groups)
            for piece in slices
        ]
    b_out_grad = lax.psum(out_bias_whole, ("seq", "img", "fsdp"))
    feats, b_out_grad = lax.optimization_barrier((feats, b_out_grad))

    part_len = sample_len // fsdp_count
    place = fsdp_index * part_len + jnp.arange(part_len, dtype=jnp.int32)
    if crossed:
        block = place // block_rows
        place = (block ^ (seq_index % stride)) * block_rows + place % block_rows
    row, mask = lookup(place)
    values = feats.at[row].get(mode="promise_in_bounds").astype(jnp.float32)
    row_mean = jnp.mean(values, axis=1, keepdims=True)
    centred = values - row_mean
    row_var = jnp.mean(centred * centred, axis=1, keepdims=True)
    normed = centred * lax.rsqrt(row_var + 1e-05)
    normed_in = (normed * ln_gain + ln_bias).astype(jnp.bfloat16)
    preact = jnp.dot(normed_in, w_in_full, preferred_element_type=jnp.float32) + in_bias
    activ, slope = gelu_parts(preact)
    hidden = jnp.where(mask[:, None], activ, 0.0).astype(jnp.bfloat16)
    slope = jnp.where(mask[:, None], slope, 0.0)
    if fsdp_count == 2:
        other = shift(hidden, "fsdp", 1)
        first = fsdp_index == 0
        hidden_full = jnp.concatenate(
            [jnp.where(first, hidden, other), jnp.where(first, other, hidden)], axis=0
        )
    else:
        hidden_full = lax.all_gather(hidden, "fsdp", axis=0, tiled=True)

    w_out_grads = []
    hidden_part = 0.0
    hidden_full, pieces[0] = lax.optimization_barrier((hidden_full, pieces[0]))
    for c in range(CHUNKS):
        piece = pieces[c]
        part = contract(hidden_full, piece, 0, 0)
        part = part.reshape(samples, img_count, block_hid // img_count, width)
        part = scatter_sum(part.transpose(1, 0, 2, 3), "img")
        w_out_grads.append(part)
        hidden_part = hidden_part + contract(
            piece, w_out_full[:, c * width : (c + 1) * width], 1, 1
        )

    hidden_grad = scatter_sum(hidden_part.reshape(fsdp_count, part_len, hid), "fsdp")
    preact_grad = (hidden_grad * slope).astype(jnp.bfloat16)
    in_part = contract(normed_in, preact_grad, 0, 0)
    in_part = in_part.reshape(img_count, fsdp_count, -1, samples, block_hid)
    in_part = scatter_sum(in_part.transpose(1, 0, 2, 3, 4), "fsdp")
    in_part = scatter_sum(in_part, "img")

    b_in_part = jnp.sum(preact_grad, axis=0, dtype=jnp.float32)
    normed_grad = contract(preact_grad, w_in_full, 1, 1)
    gain_part = jnp.sum(normed_grad * normed, axis=0)
    bias_part = jnp.sum(normed_grad, axis=0)
    hidden_bias = jnp.zeros((seq_count, block_hid), jnp.float32)
    for k in range(samples):
        owner = (seq_index - k * stride + seq_count) % seq_count
        hidden_bias = lax.dynamic_update_slice(
            hidden_bias, b_in_part[None, k * block_hid : (k + 1) * block_hid], (owner, 0)
        )
    gain_grad, bias_grad, b_in_grad = lax.psum(
        (gain_part, bias_part, hidden_bias.reshape(-1)), ("seq", "img", "fsdp")
    )
    w_in_grad = sample_sum(in_part.transpose(1, 0, 2), stride, gain_grad)
    w_out_grad = jnp.concatenate(
        [sample_sum(part, stride, gain_grad) for part in w_out_grads], axis=1
    )
    return (w_in_grad, b_in_grad, w_out_grad, b_out_grad, gain_grad, bias_grad)


def kernel_body(
    dims,
    counts_ref,
    pos_ref,
    feats_ref,
    gain_ref,
    bias_ref,
    wi_ref,
    bin_ref,
    wo_ref,
    lm_ref,
    wo_hbm,
    wi_hbm,
    gain_hbm,
    bias_hbm,
    b_in_hbm,
    b_out_hbm,
    L,
    W,
    WI,
    F,
    NT,
    V,
    MEAN,
    RSTD,
    SL,
    HT,
    HP,
    PG,
    HR,
    YS,
    YR,
    ZS,
    ZR,
    GP,
    WS,
    WR,
    WYS,
    WYR,
    WZS,
    WZR,
    PB,
    ACC,
    SV,
    AR,
    wo_out,
    wi_out,
    small_out,
    out_sem,
    send_sem,
    recv_sem,
    local_sem,
):
    rows, half, hb, dv, frows, tokens, seq_count, samples, images = dims
    stride = seq_count // samples
    span = stride * rows
    part = span // 2
    hid = samples * hb
    hh = hb // 2
    dvh = dv // 2
    dvq = dv // 4
    ck = half // PIECES
    seq = lax.axis_index("seq")
    img = lax.axis_index("img")
    core = lax.axis_index("fsdp")

    def flip(value, bits):
        for bit in (1, 2, 4):
            if bits & bit:
                value = value + bit - 2 * bit * ((value // bit) % 2)
        return value

    def device(bits=0, y=0, c=0):
        return (
            flip(seq, bits),
            1 - img if y else img,
            1 - core if c else core,
        )

    z1 = device(2)
    z2 = device(4)
    z3 = device(6)
    xn = device(1)
    yn = device(y=1)
    sib = device(c=1)

    names = {}

    def slot(name, count=1):
        if name not in names:
            names[name] = sum(c for _, c in names.values()), count
        return names[name][0]

    def remote(src, dst, target, recv, send=None, k=0, count=1):
        return pltpu.make_async_remote_copy(
            src_ref=src,
            dst_ref=dst,
            send_sem=send_sem.at[slot(send or recv, count) + k],
            recv_sem=recv_sem.at[slot(recv, count) + k],
            device_id=target,
            device_id_type=pl.DeviceIdType.MESH,
        )

    started = []

    def start(*args, **kwargs):
        copy = remote(*args, **kwargs)
        copy.start()
        started.append(copy)

    def aligned(value, unit):
        return pl.multiple_of(value, unit)

    def feat_block(bits, c):
        return F.at[pl.ds(aligned((flip(seq, bits) * 2 + c) * frows, 16), frows)]

    inside = seq % stride
    sample = seq // stride
    bounds = [counts_ref[0, 0] * 0]
    for s in range(samples):
        bounds.append(bounds[-1] + counts_ref[0, s])
    low = bounds[0]
    high = bounds[1]
    for s in range(1, samples):
        low = jnp.where(sample == s, bounds[s], low)
        high = jnp.where(sample == s, bounds[s + 1], high)
    begins = []
    for n in range(images):
        here = jnp.where(n >= low, jnp.where(n < high, 1, 0), 0)
        begins.append(jnp.where(here == 1, pos_ref[0, n * PATCH], 2 * span))

    def lookup(place):
        row = jnp.full(place.shape, -1, jnp.int32)
        for n in range(images):
            offset = place - begins[n]
            match = jnp.logical_and(offset >= 0, offset < PATCH)
            row = jnp.where(match, offset + n * PATCH, row)
        return row

    lanes = SV.shape[2]
    gain_row, bias_row = 0, dv // lanes
    b_in_row = 2 * (dv // lanes)
    b_out_row = b_in_row + seq_count * (hb // lanes)

    def put_small(row, value):
        for m in range(value.shape[1] // lanes):
            SV[0, pl.ds(row + m, 1)] = value[:, m * lanes : (m + 1) * lanes]

    def own_sums():
        place = inside * rows + lax.broadcasted_iota(jnp.int32, (rows, 1), 0)
        own_kept = jnp.where(lookup(place) >= 0, 1.0, 0.0).astype(F32)
        for m in range(half // hb):
            block = L[pl.ds(0, rows), pl.ds(m * hb, hb)].astype(F32) * own_kept
            total = jnp.sum(block, axis=0, keepdims=True)
            put_small(b_out_row + core * (half // lanes) + m * (hb // lanes), total)

    barrier = pltpu.get_barrier_semaphore()
    for target in (z1, z2, z3, xn, yn, sib):
        pl.semaphore_signal(
            barrier, inc=1, device_id=target, device_id_type=pl.DeviceIdType.MESH
        )

    locals_ = [
        pltpu.make_async_copy(feats_ref, feat_block(0, core), local_sem.at[0]),
        pltpu.make_async_copy(
            wi_ref, WI.at[0, pl.ds(aligned(core * dvh, dvh), dvh)], local_sem.at[1]
        ),
        pltpu.make_async_copy(lm_ref, L.at[pl.ds(0, rows)], local_sem.at[2]),
        pltpu.make_async_copy(wo_ref, W.at[0], local_sem.at[3]),
    ]
    for copy in locals_:
        copy.start()
    pl.semaphore_wait(barrier, 6)

    def lm_piece(k, index):
        columns = pl.ds(aligned(k * ck, ck), ck)
        return L.at[pl.ds(index * rows, rows), columns]

    def lm_own(k):
        return lm_ref.at[:, pl.ds(aligned(k * ck, ck), ck)]

    def x_copy(k):
        return remote(lm_own(k), lm_piece(k, 1), xn, "X", k=k, count=PIECES)

    def z_copy(k):
        return remote(lm_own(k), lm_piece(k, 2), z1, "Z", k=k, count=PIECES)

    def d_copy(k):
        return remote(lm_piece(k, 2), lm_piece(k, 3), xn, "D", k=k, count=PIECES)

    zseq = seq // 2
    inner = (zseq + 1) // 2 == 1

    def ht_copy(t):
        return remote(ht_piece(t, core), ht_piece(t, core), sib, "HT", k=t, count=stride)

    def hr_copy(s):
        here = pl.ds(aligned(s * tile, tile), tile)
        return remote(PG.at[here], HR.at[here], sib, "HR", k=s, count=stride)
    wi_rows = pl.ds(aligned(img * dvq, dvq), dvq)
    wi_mine = WI.at[1, pl.ds(aligned(core * dvh + img * dvq, dvq), dvq)]
    wi_other = WI.at[1, pl.ds(aligned(core * dvh + (1 - img) * dvq, dvq), dvq)]
    quarter = hh // 2

    def wo_piece(y, n):
        return pl.ds(aligned(y * hh + n * quarter, quarter), quarter)

    def hand_wo(n):
        piece = W.at[1, wo_piece(img, n)]
        remote(piece, piece, z2, f"WZ{n}").wait_recv()
        remote(piece, piece, yn, f"WY{n}").start()

    def ht_piece(s, c):
        return HT.at[:, pl.ds(aligned(s * rows + c * tile, tile), tile)]

    tile = rows // 2

    start(feats_ref, feat_block(0, core), z1, "F2")
    start(bin_ref, PB, z2, "BZ")
    wi_copy = remote(wi_ref.at[wi_rows], wi_mine, z2, "WIZ")
    wo_copies = [
        remote(wo_ref.at[wo_piece(img, n)], W.at[1, wo_piece(img, n)], z2, f"WZ{n}")
        for n in range(2)
    ]
    outer = 1 - (zseq + 1) // 2 % 2 == 1

    @pl.when(inner)
    def _():
        wi_copy.start()

    for k in range(EARLY_Z):
        z_copy(k).start()

    @pl.when(outer)
    def _():
        z_copy(EARLY_Z).start()
        wi_copy.start()
        for copy in wo_copies:
            copy.start()
        for k in range(EARLY_Z + 1, PIECES):
            z_copy(k).start()

    start(feats_ref, feat_block(0, core), xn, "F1")
    x_copy(0).start()
    start(feats_ref, feat_block(0, core), sib, "S0")
    start(wi_ref, WI.at[0, pl.ds(aligned(core * dvh, dvh), dvh)], sib, "WIS0")

    def arrive(bits, name):
        remote(feats_ref, feat_block(bits, core), xn, name).wait_recv()

    def hand_x(bits):
        block = feat_block(bits, core)
        start(block, block, xn, f"F{bits + 1}")

    def hand_sib(bits):
        block = feat_block(bits, core)
        start(block, block, sib, f"S{bits}")

    arrive(2, "F2")
    locals_[0].wait()
    own_block, pair_block = feat_block(0, core), feat_block(2, core)
    far_block, near_block = feat_block(4, core), feat_block(6, core)
    cut_own = remote(own_block, own_block, z3, "F6", send="C0")
    cut_pair = remote(pair_block, pair_block, z3, "F4", send="C1")
    back_near = remote(near_block, near_block, z1, "F4", send="C2")
    back_far = remote(far_block, far_block, z1, "F6", send="C3")

    @pl.when(inner)
    def _():
        cut_own.start()
        cut_pair.start()
        for copy in wo_copies:
            copy.start()

    hand_x(2)
    hand_sib(2)
    x_copy(1).start()

    @pl.when(outer)
    def _():
        for k in range(2, EARLY_X):
            x_copy(k).start()

    HP[...] = jnp.zeros(HP.shape, F32)
    ACC[...] = jnp.zeros(ACC.shape, F32)
    SV[0] = jnp.zeros(SV.shape[1:], F32)
    locals_[2].wait()
    own_sums()
    arrive(4, "F4")
    arrive(6, "F6")

    @pl.when(inner)
    def _():
        back_near.start()
        back_far.start()
        for k in range(EARLY_Z, PIECES):
            z_copy(k).start()

    for bits in (4, 6):
        hand_x(bits)
        hand_sib(bits)

    @pl.when(inner)
    def _():
        for k in range(2, EARLY_X):
            x_copy(k).start()

    for k in range(EARLY_Z):
        z_copy(k).wait_recv()
        d_copy(k).start()
    wi_copy.wait_recv()
    start(wi_mine, wi_mine, yn, "WIY")
    start(wi_mine, wi_mine, sib, "WIS1")
    for bits in (1, 3, 5, 7):
        arrive(bits, f"F{bits}")
        hand_sib(bits)
    remote(wi_other, wi_other, yn, "WIY").wait_recv()
    start(wi_other, wi_other, sib, "WIS2")
    for k in range(EARLY_Z, AHEAD_D):
        z_copy(k).wait_recv()
        d_copy(k).start()
    for k in range(EARLY_X, AHEAD_X):
        x_copy(k).start()
    remote(bin_ref, PB, z2, "BZ").wait_recv()
    remote(
        wi_ref, WI.at[0, pl.ds(aligned((1 - core) * dvh, dvh), dvh)], sib, "WIS0"
    ).wait_recv()
    for name, y in (("WIS1", img), ("WIS2", 1 - img)):
        piece = WI.at[1, pl.ds(aligned((1 - core) * dvh + y * dvq, dvq), dvq)]
        remote(piece, piece, sib, name).wait_recv()
    for bits in range(8):
        block = feat_block(bits, 1 - core)
        remote(block, block, sib, f"S{bits}").wait_recv()
    for copy in (locals_[1], locals_[3]):
        copy.wait()

    @pl.loop(0, stride)
    def _(t):
        block = inside + t % 2 - 2 * (t % 2) * (inside % 2)
        block = block + 2 * (t // 2) - 4 * (t // 2) * ((block // 2) % 2)
        first = block * rows + core * tile
        place = first + lax.broadcasted_iota(jnp.int32, (tile, 1), 0)
        row = lookup(place)
        kept = jnp.where(row >= 0, 1.0, 0.0).astype(F32)
        wanted = lax.broadcasted_iota(jnp.int32, (tile, tokens), 1) == row
        chosen = jnp.where(wanted, 1.0, 0.0).astype(BF16)
        values = jnp.dot(chosen, F[...], preferred_element_type=F32)
        here = pl.ds(aligned(t * tile, tile), tile)
        V[here] = values.astype(BF16)
        mean = jnp.mean(values, axis=1, keepdims=True)
        centred = values - mean
        rstd = lax.rsqrt(jnp.mean(centred * centred, axis=1, keepdims=True) + 1e-05)
        MEAN[here] = mean
        RSTD[here] = rstd
        scaled = centred * rstd * gain_ref[...] + bias_ref[...]
        normed_in = scaled.astype(BF16)
        NT[:, here] = scaled.T.astype(BF16)
        for g in range(samples):
            shift_row = bin_ref[...] if g == 0 else PB[...]
            preact = jnp.dot(normed_in, WI[g], preferred_element_type=F32) + shift_row
            activ, slope = gelu_parts(preact)
            columns = pl.ds(g * hb, hb)
            SL[here, columns] = slope * kept
            HT[columns, pl.ds(aligned(t * rows + core * tile, tile), tile)] = (
                (activ * kept).T.astype(BF16)
            )
        ht_copy(t).start()

    hand_wo(0)
    for t in range(stride):
        remote(ht_piece(t, 1 - core), ht_piece(t, 1 - core), sib, "HT", k=t, count=stride).wait_recv()
    def y_copy(k):
        columns = pl.ds(aligned(k * ck, ck), ck)
        return remote(YS.at[:, columns], YR.at[:, columns], yn, "YK", k=k, count=PIECES)

    def zk_copy(k):
        columns = pl.ds(aligned(k * ck, ck), ck)
        return remote(ZS.at[:, columns], ZR.at[:, columns], z2, "ZK", k=k, count=PIECES)

    def weight_grad(k):
        columns = pl.ds(aligned(k * ck, ck), ck)
        piece = L[:, columns]
        for g in range(samples):
            mine = pl.ds(aligned(g * hb + img * hh, hh), hh)
            other = pl.ds(aligned(g * hb + (1 - img) * hh, hh), hh)
            sent = jnp.dot(HT[other], piece, preferred_element_type=F32)
            YS[pl.ds(g * hh, hh), columns] = sent.astype(BF16)
            kept = jnp.dot(HT[mine], piece, preferred_element_type=F32)
            if g == 0:
                wo_out[:, columns] = kept
            else:
                GP[:, columns] = kept
        y_copy(k).start()

    def hidden_part(k, s, g, low, size):
        columns = pl.ds(aligned(k * ck, ck), ck)
        HP[s, :, pl.ds(aligned(g * hb + low, hh), size)] += lax.dot_general(
            L[pl.ds(aligned(s * rows, rows), rows), columns],
            W[g, pl.ds(aligned(low, hh), size), columns],
            (((1,), (1,)), ((), ())),
            preferred_element_type=F32,
        )

    def half_rows(c):
        return pl.ds(aligned(c * tile, tile), tile)

    def exchange(s):
        PG[pl.ds(aligned(s * tile, tile), tile)] = HP[s, half_rows(1 - core)].astype(BF16)
        hr_copy(s).start()

    def preact_grad(s):
        copy = hr_copy(s)
        copy.wait()
        here = pl.ds(s * tile, tile)
        grad = HP[s, half_rows(core)] + HR[here].astype(F32)
        rounded = (grad * SL[here]).astype(BF16)
        PG[here] = rounded
        ACC[pl.ds(0, 1)] += jnp.sum(rounded.astype(F32), axis=0, keepdims=True)

    def over_img(k):
        columns = pl.ds(aligned(k * ck, ck), ck)
        y_copy(k).wait_recv()
        wo_out[:, columns] += YR[pl.ds(0, hh), columns].astype(F32)
        both = GP[:, columns] + YR[pl.ds(hh, hh), columns].astype(F32)
        ZS[:, columns] = both.astype(BF16)
        zk_copy(k).start()

    def over_samples(k):
        columns = pl.ds(aligned(k * ck, ck), ck)
        zk_copy(k).wait_recv()
        wo_out[:, columns] += ZR[:, columns].astype(F32)

    ACC[...] = jnp.zeros(ACC.shape, F32)

    last = stride - 1

    def hidden_parts(k, s):
        hidden_part(k, s, 0, 0, hb)
        for n in range(LATE_MINE, PIECES):

            @pl.when(k == n)
            def _():
                for late, step, y in ((LATE_MINE, 2, img), (LATE, 3, 1 - img)):
                    low = min(step * (n - late), n)
                    high = min(step * (n - late) + step, n + 1)
                    if n >= late:

                        @pl.loop(low, high)
                        def _(j):
                            for g in range(1, samples):
                                hidden_part(j, s, g, y * hh, hh)

    @pl.loop(0, PIECES)
    def _(k):
        x_copy(k).wait_recv()

        @pl.when(k == LATE)
        def _():
            for n in range(2):
                piece = W.at[1, wo_piece(1 - img, n)]
                remote(piece, piece, yn, f"WY{n}").wait_recv()

        @pl.loop(0, last)
        def _(s):
            hidden_parts(k, s)

            @pl.when(k == PIECES - 1)
            def _():
                exchange(s)

        d_copy(k).wait_recv()
        hidden_parts(k, last)

        @pl.when(k == PIECES - 1)
        def _():
            exchange(last)

        weight_grad(k)

        @pl.when(k == 2)
        def _():
            hand_wo(1)

        @pl.when(k + AHEAD_X < PIECES)
        def _():
            x_copy(k + AHEAD_X).start()

        @pl.when(k + AHEAD_D < PIECES)
        def _():
            z_copy(k + AHEAD_D).wait_recv()
            d_copy(k + AHEAD_D).start()

        @pl.when(k >= 2)
        def _():
            over_img(k - 2)


    over_img(PIECES - 2)
    for s in range(last):
        preact_grad(s)
    preact_grad(last)

    def first_grad(block):
        lines = pl.ds(aligned(block * dvq, dvq), dvq)
        return jnp.dot(NT[lines], PG[...], preferred_element_type=F32)

    for y in range(2):
        WS[y] = first_grad(2 * y + 1 - core).astype(BF16)
    start(WS, WR, sib, "WG")
    kept_rows = [pl.ds(y * dvq, dvq) for y in range(2)]
    for y in range(2):
        HP[0, kept_rows[y]] = first_grad(2 * y + core)
    remote(WS, WR, sib, "WG").wait_recv()
    other_rows = pl.ds(aligned((1 - img) * dvq, dvq), dvq)
    mine_rows = pl.ds(aligned(img * dvq, dvq), dvq)
    WYS[...] = (HP[0, other_rows] + WR[1 - img].astype(F32)).astype(BF16)
    own_cols = pl.ds(0, hb)
    far_cols = [pl.ds(hb + n * (hb // 2), hb // 2) for n in range(2)]
    for n in range(2):
        start(WYS.at[:, far_cols[n]], WYR.at[:, far_cols[n]], yn, f"WYF{n}")
    start(WYS.at[:, own_cols], WYR.at[:, own_cols], yn, "WYO")
    over_img(PIECES - 1)

    @pl.loop(0, part // tile)
    def _(t):
        here = pl.ds(aligned(t * tile, tile), tile)
        grad = jnp.zeros((tile, dv), F32)
        for g in range(samples):
            grad = grad + lax.dot_general(
                PG[here, pl.ds(g * hb, hb)],
                WI[g],
                (((1,), (1,)), ((), ())),
                preferred_element_type=F32,
            )
        normed = (V[here].astype(F32) - MEAN[here]) * RSTD[here]
        ACC[pl.ds(1, 1)] += jnp.sum(grad * normed, axis=0, keepdims=True)
        ACC[pl.ds(2, 1)] += jnp.sum(grad, axis=0, keepdims=True)

    put_small(gain_row, ACC[pl.ds(1, 1)][:, :dv])
    put_small(bias_row, ACC[pl.ds(2, 1)][:, :dv])
    sums = ACC[pl.ds(0, 1)]
    for g in range(samples):
        put_small(
            b_in_row + flip(seq, 4 * g) * (hb // lanes), sums[:, g * hb : (g + 1) * hb]
        )

    def small_start(n, target):
        start(SV.at[n], AR.at[n], target, f"AR{n}")

    def small_end(n):
        remote(SV.at[n], AR.at[n], sib, f"AR{n}").wait_recv()
        return SV[n] + AR[n]

    def over_far(n):
        local = pl.ds(n * (hb // 2), hb // 2)
        columns = far_cols[n]
        remote(WYS.at[:, columns], WYR.at[:, columns], yn, f"WYF{n}").wait_recv()
        total = HP[0, mine_rows, columns] + WR[img, :, columns].astype(F32)
        WZS[:, local] = (total + WYR[:, columns].astype(F32)).astype(BF16)
        start(WZS.at[:, local], WZR.at[:, local], z2, f"WZS{n}")

    small_start(0, sib)
    SV[1] = small_end(0)
    small_start(1, z1)
    over_far(0)
    SV[2] = small_end(1)
    small_start(2, z2)
    over_far(1)
    SV[3] = small_end(2)
    small_start(3, yn)
    remote(WYS.at[:, own_cols], WYR.at[:, own_cols], yn, "WYO").wait_recv()
    wi_out[...] = (HP[0, mine_rows, own_cols] + WR[img, :, own_cols].astype(F32)
                   + WYR[:, own_cols].astype(F32))
    SV[4] = small_end(3)
    small_start(4, xn)
    def wo_store(k):
        columns = pl.ds(aligned(k * ck, ck), ck)
        return pltpu.make_async_copy(
            wo_out.at[:, columns], wo_hbm.at[:, columns], out_sem.at[k]
        )

    @pl.loop(0, PIECES)
    def _(k):
        over_samples(k)
        wo_store(k).start()

    for n in range(2):
        local = pl.ds(n * (hb // 2), hb // 2)
        remote(WZS.at[:, local], WZR.at[:, local], z2, f"WZS{n}").wait_recv()
        wi_out[:, local] += WZR[:, local].astype(F32)
    small_out[...] = small_end(4)
    stores = [pltpu.make_async_copy(wi_out, wi_hbm, out_sem.at[PIECES])]
    row = 0
    for n, ref in enumerate((gain_hbm, bias_hbm, b_in_hbm, b_out_hbm)):
        piece = small_out.at[pl.ds(row, ref.shape[0])]
        stores.append(pltpu.make_async_copy(piece, ref, out_sem.at[PIECES + 1 + n]))
        row += ref.shape[0]
    for copy in stores:
        copy.start()
    for copy in started:
        copy.wait_send()

    @pl.when(inner)
    def _():
        for copy in (cut_own, cut_pair, back_near, back_far):
            copy.wait_send()

    for n in range(2):
        piece = W.at[1, wo_piece(img, n)]
        remote(piece, piece, yn, f"WY{n}").wait_send()
    for t in range(stride):
        ht_copy(t).wait_send()
    for copy in (wi_copy, *wo_copies):
        copy.wait_send()

    @pl.loop(0, PIECES)
    def _(k):
        for copy in (x_copy, z_copy, d_copy, y_copy, zk_copy):
            copy(k).wait_send()

    @pl.loop(0, PIECES)
    def _(k):
        wo_store(k).wait()

    for copy in stores:
        copy.wait()


def finish_body(ins, outs, held, sems):
    copies = []
    for n, (source, place) in enumerate(zip(ins, held)):
        copy = pltpu.make_async_copy(source, place, sems.at[0, n])
        copy.start()
        copies.append(copy)
    later = []
    for n, (place, target) in enumerate(zip(held, outs)):
        copies[n].wait()
        copy = pltpu.make_async_copy(place, target, sems.at[1, n])
        copy.start()
        later.append(copy)
    for copy in later:
        copy.wait()


def finish(values):
    count = len(values)
    hbm = pl.BlockSpec(memory_space=pl.ANY)

    def body(*refs):
        finish_body(refs[:count], refs[count : 2 * count], refs[2 * count : -1], refs[-1])

    return pl.pallas_call(
        body,
        out_shape=[jax.ShapeDtypeStruct(v.shape, v.dtype) for v in values],
        in_specs=[hbm] * count,
        out_specs=[hbm] * count,
        scratch_shapes=[pltpu.VMEM(v.shape, v.dtype) for v in values]
        + [pltpu.SemaphoreType.DMA((2, count))],
    )(*values)


def per_device_kernel(
    vision_feats, ln_gain, ln_bias, w_in, b_in, w_out, lm_grad, image_counts, token_pos
):
    seq_count = lax.axis_size("seq")
    _, rows, half = lm_grad.shape
    hb = w_out.shape[0]
    dv = ln_gain.shape[0]
    frows = vision_feats.shape[1]
    tokens = token_pos.shape[1]
    samples = image_counts.shape[1]
    stride = seq_count // samples
    span = stride * rows
    part = span // 2
    hid = samples * hb
    images = tokens // PATCH
    lanes = 128
    small = (2 * dv + seq_count * hb + 2 * half) // lanes
    dims = (rows, half, hb, dv, frows, tokens, seq_count, samples, images)
    vmem = pl.BlockSpec(memory_space=pltpu.VMEM)
    smem = pl.BlockSpec(memory_space=pltpu.SMEM)
    hbm = pl.BlockSpec(memory_space=pl.ANY)
    wo, wi, *sums = pl.pallas_call(
        functools.partial(kernel_body, dims),
        out_shape=(
            jax.ShapeDtypeStruct((hb // 2, half), F32),
            jax.ShapeDtypeStruct((dv // 4, hb), F32),
            jax.ShapeDtypeStruct((dv // lanes, lanes), F32),
            jax.ShapeDtypeStruct((dv // lanes, lanes), F32),
            jax.ShapeDtypeStruct((seq_count * hb // lanes, lanes), F32),
            jax.ShapeDtypeStruct((2 * half // lanes, lanes), F32),
        ),
        in_specs=[smem, smem, hbm, vmem, vmem, hbm, vmem, hbm, hbm],
        out_specs=[hbm] * 6,
        scratch_shapes=[
            pltpu.VMEM((span, half), BF16),
            pltpu.VMEM((samples, hb, half), BF16),
            pltpu.VMEM((samples, dv, hb), BF16),
            pltpu.VMEM((tokens, dv), BF16),
            pltpu.VMEM((dv, part), BF16),
            pltpu.VMEM((part, dv), BF16),
            pltpu.VMEM((part, 1), F32),
            pltpu.VMEM((part, 1), F32),
            pltpu.VMEM((part, hid), F32),
            pltpu.VMEM((hid, span), BF16),
            pltpu.VMEM((stride, rows, hid), F32),
            pltpu.VMEM((part, hid), BF16),
            pltpu.VMEM((part, hid), BF16),
            pltpu.VMEM((hb, half), BF16),
            pltpu.VMEM((hb, half), BF16),
            pltpu.VMEM((hb // 2, half), BF16),
            pltpu.VMEM((hb // 2, half), BF16),
            pltpu.VMEM((hb // 2, half), F32),
            pltpu.VMEM((2, dv // 4, hid), BF16),
            pltpu.VMEM((2, dv // 4, hid), BF16),
            pltpu.VMEM((dv // 4, hid), BF16),
            pltpu.VMEM((dv // 4, hid), BF16),
            pltpu.VMEM((dv // 4, hb), BF16),
            pltpu.VMEM((dv // 4, hb), BF16),
            pltpu.VMEM((1, hb), F32),
            pltpu.VMEM((8, max(hid, dv)), F32),
            pltpu.VMEM((5, small, lanes), F32),
            pltpu.VMEM((5, small, lanes), F32),
            pltpu.VMEM((hb // 2, half), F32),
            pltpu.VMEM((dv // 4, hb), F32),
            pltpu.VMEM((small, lanes), F32),
            pltpu.SemaphoreType.DMA((PIECES + 5,)),
            pltpu.SemaphoreType.DMA((96,)),
            pltpu.SemaphoreType.DMA((96,)),
            pltpu.SemaphoreType.DMA((4,)),
        ],
        compiler_params=pltpu.CompilerParams(
            collective_id=0, has_side_effects=True, vmem_limit_bytes=67043328
        ),
    )(
        image_counts,
        token_pos,
        vision_feats[0],
        ln_gain[None],
        ln_bias[None],
        w_in,
        b_in[None],
        w_out,
        lm_grad[0],
    )
    wo, wi, *sums = finish((wo, wi, *sums))
    gain_grad, bias_grad, b_in_grad, b_out_grad = (value.reshape(-1) for value in sums)
    return (wi, b_in_grad, wo, b_out_grad, gain_grad, bias_grad)


def dispatch(mesh, *args):
    sizes = (mesh.shape["seq"], mesh.shape["img"], mesh.shape["fsdp"])
    if sizes == (8, 2, 2) and args[7].shape[1] == 2:
        return per_device_kernel(*args)
    return per_device(*args)


def solution(mesh):
    return jax.shard_map(
        functools.partial(dispatch, mesh),
        mesh=mesh,
        in_specs=(
            P("img", ("seq", "fsdp"), None),
            P(),
            P(),
            P("fsdp", "seq"),
            P("seq"),
            P("seq", "fsdp"),
            P("img", "seq", "fsdp"),
            P("img", None),
            P("img", None),
        ),
        out_specs=(
            P(("img", "fsdp"), "seq"),
            P(),
            P(("seq", "img"), "fsdp"),
            P(),
            P(),
            P(),
        ),
        check_vma=False,
    )
```

```python
import functools

import jax
import jax.numpy as jnp
from jax import lax
from jax.experimental import pallas as pl
from jax.experimental.pallas import tpu as pltpu
from jax.sharding import PartitionSpec as P

PATCH = 576
CHUNKS = 2
PIECES = 8
EARLY_X = 4
EARLY_D = 2
LATE_X = 6
LATE_MINE = 3
LATE = 4
BF16 = jnp.bfloat16
F32 = jnp.float32


def gelu_parts(preact):
    cumul = 0.5 * (1.0 + lax.erf(preact * 0.7071067811865476))
    density = jnp.exp(-0.5 * preact * preact) * 0.3989422804014327
    return (preact * cumul, cumul + preact * density)


def contract(left, right, left_dim, right_dim):
    return lax.dot_general(
        left, right, (((left_dim,), (right_dim,)), ((), ())), preferred_element_type=jnp.float32
    )


def shift(value, axis, amount):
    count = lax.axis_size(axis)
    return lax.ppermute(value, axis, [(i, (i + amount) % count) for i in range(count)])


def flip(value, bit):
    count = lax.axis_size("seq")
    return lax.ppermute(value, "seq", [(i, i ^ bit) for i in range(count)])


def pick(value, index, axis):
    return lax.dynamic_index_in_dim(value, index, axis=axis, keepdims=False)


def scatter_sum(value, axis):
    count = lax.axis_size(axis)
    index = lax.axis_index(axis)
    if count > 2:
        return lax.psum_scatter(value, axis, scatter_dimension=0, tiled=False)
    if count == 1:
        return value[0]
    sent = pick(value, 1 - index, 0).astype(jnp.bfloat16)
    return pick(value, index, 0) + shift(sent, axis, 1).astype(jnp.float32)


def sample_sum(value, stride, after):
    total, _ = lax.optimization_barrier((value[0], after))
    for k in range(1, value.shape[0]):
        moved = shift(value[k].astype(jnp.bfloat16), "seq", -k * stride)
        total = total + moved.astype(jnp.float32)
    return total


def per_device(vision_feats, ln_gain, ln_bias, w_in, b_in, w_out, lm_grad, image_counts, token_pos):
    seq_count = lax.axis_size("seq")
    seq_index = lax.axis_index("seq")
    img_count = lax.axis_size("img")
    fsdp_count = lax.axis_size("fsdp")
    fsdp_index = lax.axis_index("fsdp")
    lm_block = lm_grad[0]
    block_rows, half_width = lm_block.shape
    counts = image_counts[0]
    samples = counts.shape[0]
    stride = seq_count // samples
    sample_len = stride * block_rows
    own_sample = seq_index // stride
    positions = token_pos[0]
    row_count = positions.shape[0]
    images = row_count // PATCH
    starts = positions.reshape(images, PATCH)[:, 0]
    bounds = jnp.cumsum(counts)
    image_index = jnp.arange(images, dtype=jnp.int32)
    image_sample = jnp.sum((image_index[:, None] >= bounds[None, :]).astype(jnp.int32), axis=1)
    in_sample = image_sample == own_sample

    def lookup(place):
        offset = place[:, None] - starts[None, :]
        match = in_sample[None, :] & (offset >= 0) & (offset < PATCH)
        row = jnp.sum(jnp.where(match, offset + image_index[None, :] * PATCH, 0), axis=1)
        return row, jnp.any(match, axis=1)

    own_place = (seq_index % stride) * block_rows + jnp.arange(block_rows, dtype=jnp.int32)
    own_mask = lookup(own_place)[1].astype(jnp.bfloat16)
    out_bias_half = jnp.dot(own_mask[None, :], lm_block, preferred_element_type=jnp.float32)[0]
    out_bias_whole = lax.dynamic_update_slice_in_dim(
        jnp.zeros((half_width * fsdp_count,), jnp.float32),
        out_bias_half,
        fsdp_index * half_width,
        0,
    )

    feats = lax.all_gather(vision_feats[0], ("seq", "fsdp"), axis=0, tiled=True)

    in_blocks = [w_in] + [shift(w_in, "seq", k * stride) for k in range(1, samples)]
    in_bias = jnp.concatenate([b_in] + [shift(b_in, "seq", k * stride) for k in range(1, samples)])
    w_in_half = jnp.concatenate(in_blocks, axis=1)
    w_in_full = lax.all_gather(w_in_half, "fsdp", axis=0, tiled=True)
    w_out_later, _ = lax.optimization_barrier((w_out, w_in_half))
    w_out_full = jnp.concatenate(
        [w_out] + [shift(w_out_later, "seq", k * stride) for k in range(1, samples)], axis=0
    )
    hid = in_bias.shape[0]
    block_hid = hid // samples

    groups = [[s * stride + i for i in range(stride)] for s in range(samples)]
    width = half_width // CHUNKS
    slices = [lm_block[:, c * width : (c + 1) * width] for c in range(CHUNKS)]
    crossed = stride == 4
    if crossed:
        pieces = []
        for piece in slices:
            far = flip(piece, 2)
            near = flip(piece, 1)
            pieces.append(jnp.concatenate([piece, near, far, flip(far, 1)], axis=0))
    else:
        pieces = [
            lax.all_gather(piece, "seq", axis=0, tiled=True, axis_index_groups=groups)
            for piece in slices
        ]
    b_out_grad = lax.psum(out_bias_whole, ("seq", "img", "fsdp"))
    feats, b_out_grad = lax.optimization_barrier((feats, b_out_grad))

    part_len = sample_len // fsdp_count
    place = fsdp_index * part_len + jnp.arange(part_len, dtype=jnp.int32)
    if crossed:
        block = place // block_rows
        place = (block ^ (seq_index % stride)) * block_rows + place % block_rows
    row, mask = lookup(place)
    values = feats.at[row].get(mode="promise_in_bounds").astype(jnp.float32)
    row_mean = jnp.mean(values, axis=1, keepdims=True)
    centred = values - row_mean
    row_var = jnp.mean(centred * centred, axis=1, keepdims=True)
    normed = centred * lax.rsqrt(row_var + 1e-05)
    normed_in = (normed * ln_gain + ln_bias).astype(jnp.bfloat16)
    preact = jnp.dot(normed_in, w_in_full, preferred_element_type=jnp.float32) + in_bias
    activ, slope = gelu_parts(preact)
    hidden = jnp.where(mask[:, None], activ, 0.0).astype(jnp.bfloat16)
    slope = jnp.where(mask[:, None], slope, 0.0)
    if fsdp_count == 2:
        other = shift(hidden, "fsdp", 1)
        first = fsdp_index == 0
        hidden_full = jnp.concatenate(
            [jnp.where(first, hidden, other), jnp.where(first, other, hidden)], axis=0
        )
    else:
        hidden_full = lax.all_gather(hidden, "fsdp", axis=0, tiled=True)

    w_out_grads = []
    hidden_part = 0.0
    hidden_full, pieces[0] = lax.optimization_barrier((hidden_full, pieces[0]))
    for c in range(CHUNKS):
        piece = pieces[c]
        part = contract(hidden_full, piece, 0, 0)
        part = part.reshape(samples, img_count, block_hid // img_count, width)
        part = scatter_sum(part.transpose(1, 0, 2, 3), "img")
        w_out_grads.append(part)
        hidden_part = hidden_part + contract(
            piece, w_out_full[:, c * width : (c + 1) * width], 1, 1
        )

    hidden_grad = scatter_sum(hidden_part.reshape(fsdp_count, part_len, hid), "fsdp")
    preact_grad = (hidden_grad * slope).astype(jnp.bfloat16)
    in_part = contract(normed_in, preact_grad, 0, 0)
    in_part = in_part.reshape(img_count, fsdp_count, -1, samples, block_hid)
    in_part = scatter_sum(in_part.transpose(1, 0, 2, 3, 4), "fsdp")
    in_part = scatter_sum(in_part, "img")

    b_in_part = jnp.sum(preact_grad, axis=0, dtype=jnp.float32)
    normed_grad = contract(preact_grad, w_in_full, 1, 1)
    gain_part = jnp.sum(normed_grad * normed, axis=0)
    bias_part = jnp.sum(normed_grad, axis=0)
    hidden_bias = jnp.zeros((seq_count, block_hid), jnp.float32)
    for k in range(samples):
        owner = (seq_index - k * stride + seq_count) % seq_count
        hidden_bias = lax.dynamic_update_slice(
            hidden_bias, b_in_part[None, k * block_hid : (k + 1) * block_hid], (owner, 0)
        )
    gain_grad, bias_grad, b_in_grad = lax.psum(
        (gain_part, bias_part, hidden_bias.reshape(-1)), ("seq", "img", "fsdp")
    )
    w_in_grad = sample_sum(in_part.transpose(1, 0, 2), stride, gain_grad)
    w_out_grad = jnp.concatenate(
        [sample_sum(part, stride, gain_grad) for part in w_out_grads], axis=1
    )
    return (w_in_grad, b_in_grad, w_out_grad, b_out_grad, gain_grad, bias_grad)


def kernel_body(
    dims,
    counts_ref,
    pos_ref,
    feats_ref,
    gain_ref,
    bias_ref,
    wi_ref,
    bin_ref,
    wo_ref,
    lm_ref,
    wo_hbm,
    wi_hbm,
    gain_hbm,
    bias_hbm,
    b_in_hbm,
    b_out_hbm,
    L,
    W,
    WI,
    F,
    NT,
    V,
    MEAN,
    RSTD,
    SL,
    HT,
    HP,
    PG,
    HR,
    YS,
    YR,
    ZS,
    ZR,
    GP,
    WS,
    WR,
    WYS,
    WYR,
    WZS,
    WZR,
    PB,
    ACC,
    SV,
    AR,
    wo_out,
    wi_out,
    small_out,
    out_sem,
    send_sem,
    recv_sem,
    local_sem,
):
    rows, half, hb, dv, frows, tokens, seq_count, samples, images = dims
    stride = seq_count // samples
    span = stride * rows
    part = span // 2
    hid = samples * hb
    hh = hb // 2
    dvh = dv // 2
    dvq = dv // 4
    ck = half // PIECES
    seq = lax.axis_index("seq")
    img = lax.axis_index("img")
    core = lax.axis_index("fsdp")

    def flip(value, bits):
        for bit in (1, 2, 4):
            if bits & bit:
                value = value + bit - 2 * bit * ((value // bit) % 2)
        return value

    def device(bits=0, y=0, c=0):
        return (
            flip(seq, bits),
            1 - img if y else img,
            1 - core if c else core,
        )

    z1 = device(2)
    z2 = device(4)
    z3 = device(6)
    xn = device(1)
    yn = device(y=1)
    sib = device(c=1)

    names = {}

    def slot(name, count=1):
        if name not in names:
            names[name] = sum(c for _, c in names.values()), count
        return names[name][0]

    def remote(src, dst, target, recv, send=None, k=0, count=1):
        return pltpu.make_async_remote_copy(
            src_ref=src,
            dst_ref=dst,
            send_sem=send_sem.at[slot(send or recv, count) + k],
            recv_sem=recv_sem.at[slot(recv, count) + k],
            device_id=target,
            device_id_type=pl.DeviceIdType.MESH,
        )

    started = []

    def start(*args, **kwargs):
        copy = remote(*args, **kwargs)
        copy.start()
        started.append(copy)

    def aligned(value, unit):
        return pl.multiple_of(value, unit)

    def feat_block(bits, c):
        return F.at[pl.ds(aligned((flip(seq, bits) * 2 + c) * frows, 16), frows)]

    inside = seq % stride
    sample = seq // stride
    bounds = [counts_ref[0, 0] * 0]
    for s in range(samples):
        bounds.append(bounds[-1] + counts_ref[0, s])
    low = bounds[0]
    high = bounds[1]
    for s in range(1, samples):
        low = jnp.where(sample == s, bounds[s], low)
        high = jnp.where(sample == s, bounds[s + 1], high)
    begins = []
    for n in range(images):
        here = jnp.where(n >= low, jnp.where(n < high, 1, 0), 0)
        begins.append(jnp.where(here == 1, pos_ref[0, n * PATCH], 2 * span))

    def lookup(place):
        row = jnp.full(place.shape, -1, jnp.int32)
        for n in range(images):
            offset = place - begins[n]
            match = jnp.logical_and(offset >= 0, offset < PATCH)
            row = jnp.where(match, offset + n * PATCH, row)
        return row

    lanes = SV.shape[2]
    gain_row, bias_row = 0, dv // lanes
    b_in_row = 2 * (dv // lanes)
    b_out_row = b_in_row + seq_count * (hb // lanes)

    def put_small(row, value):
        for m in range(value.shape[1] // lanes):
            SV[0, pl.ds(row + m, 1)] = value[:, m * lanes : (m + 1) * lanes]

    def own_sums():
        place = inside * rows + lax.broadcasted_iota(jnp.int32, (rows, 1), 0)
        own_kept = jnp.where(lookup(place) >= 0, 1.0, 0.0).astype(F32)
        for m in range(half // hb):
            block = L[pl.ds(0, rows), pl.ds(m * hb, hb)].astype(F32) * own_kept
            total = jnp.sum(block, axis=0, keepdims=True)
            put_small(b_out_row + core * (half // lanes) + m * (hb // lanes), total)

    barrier = pltpu.get_barrier_semaphore()
    for target in (z1, z2, z3, xn, yn, sib):
        pl.semaphore_signal(
            barrier, inc=1, device_id=target, device_id_type=pl.DeviceIdType.MESH
        )

    locals_ = [
        pltpu.make_async_copy(feats_ref, feat_block(0, core), local_sem.at[0]),
        pltpu.make_async_copy(
            wi_ref, WI.at[0, pl.ds(aligned(core * dvh, dvh), dvh)], local_sem.at[1]
        ),
        pltpu.make_async_copy(lm_ref, L.at[pl.ds(0, rows)], local_sem.at[2]),
        pltpu.make_async_copy(wo_ref, W.at[0], local_sem.at[3]),
    ]
    for copy in locals_:
        copy.start()
    pl.semaphore_wait(barrier, 6)

    def lm_piece(k, index):
        columns = pl.ds(aligned(k * ck, ck), ck)
        return L.at[pl.ds(index * rows, rows), columns]

    def lm_own(k):
        return lm_ref.at[:, pl.ds(aligned(k * ck, ck), ck)]

    def x_copy(k):
        return remote(lm_own(k), lm_piece(k, 1), xn, "X", k=k, count=PIECES)

    def z_copy(k):
        return remote(lm_own(k), lm_piece(k, 2), z1, "Z", k=k, count=PIECES)

    def d_copy(k):
        return remote(lm_piece(k, 2), lm_piece(k, 3), xn, "D", k=k, count=PIECES)

    zseq = seq // 2
    inner = (zseq + 1) // 2 == 1

    def ht_copy(t):
        return remote(ht_piece(t, core), ht_piece(t, core), sib, "HT", k=t, count=stride)

    def hr_copy(s):
        here = pl.ds(aligned(s * tile, tile), tile)
        return remote(PG.at[here], HR.at[here], sib, "HR", k=s, count=stride)
    wi_rows = pl.ds(aligned(img * dvq, dvq), dvq)
    wi_mine = WI.at[1, pl.ds(aligned(core * dvh + img * dvq, dvq), dvq)]
    wi_other = WI.at[1, pl.ds(aligned(core * dvh + (1 - img) * dvq, dvq), dvq)]
    quarter = hh // 2

    def wo_piece(y, n):
        return pl.ds(aligned(y * hh + n * quarter, quarter), quarter)

    def hand_wo(n):
        piece = W.at[1, wo_piece(img, n)]
        remote(piece, piece, z2, f"WZ{n}").wait_recv()
        remote(piece, piece, yn, f"WY{n}").start()

    def ht_piece(s, c):
        return HT.at[:, pl.ds(aligned(s * rows + c * tile, tile), tile)]

    tile = rows // 2

    start(feats_ref, feat_block(0, core), z1, "F2")
    start(bin_ref, PB, z2, "BZ")
    wi_copy = remote(wi_ref.at[wi_rows], wi_mine, z2, "WIZ")
    wo_copies = [
        remote(wo_ref.at[wo_piece(img, n)], W.at[1, wo_piece(img, n)], z2, f"WZ{n}")
        for n in range(2)
    ]
    outer = 1 - (zseq + 1) // 2 % 2 == 1

    @pl.when(inner)
    def _():
        wi_copy.start()

    z_copy(0).start()

    @pl.when(outer)
    def _():
        for k in range(1, 3):
            z_copy(k).start()
        wi_copy.start()
        wo_copies[0].start()
        for k in range(3, PIECES - 1):
            z_copy(k).start()
        wo_copies[1].start()
        z_copy(PIECES - 1).start()

    start(feats_ref, feat_block(0, core), xn, "F1")
    x_copy(0).start()
    start(feats_ref, feat_block(0, core), sib, "S0")
    start(wi_ref, WI.at[0, pl.ds(aligned(core * dvh, dvh), dvh)], sib, "WIS0")

    def arrive(bits, name):
        remote(feats_ref, feat_block(bits, core), xn, name).wait_recv()

    def hand_x(bits):
        block = feat_block(bits, core)
        start(block, block, xn, f"F{bits + 1}")

    def hand_sib(bits):
        block = feat_block(bits, core)
        start(block, block, sib, f"S{bits}")

    arrive(2, "F2")
    locals_[0].wait()
    own_block, pair_block = feat_block(0, core), feat_block(2, core)
    far_block, near_block = feat_block(4, core), feat_block(6, core)
    cut_own = remote(own_block, own_block, z3, "F6", send="C0")
    cut_pair = remote(pair_block, pair_block, z3, "F4", send="C1")
    back_near = remote(near_block, near_block, z1, "F4", send="C2")
    back_far = remote(far_block, far_block, z1, "F6", send="C3")

    @pl.when(inner)
    def _():
        cut_own.start()
        cut_pair.start()

    hand_x(2)
    hand_sib(2)
    x_copy(1).start()

    @pl.when(outer)
    def _():
        for k in range(2, EARLY_X):
            x_copy(k).start()

    HP[...] = jnp.zeros(HP.shape, F32)
    ACC[...] = jnp.zeros(ACC.shape, F32)
    SV[0] = jnp.zeros(SV.shape[1:], F32)
    locals_[2].wait()
    own_sums()
    arrive(4, "F4")
    arrive(6, "F6")

    @pl.when(inner)
    def _():
        back_near.start()
        back_far.start()
        for copy in wo_copies:
            copy.start()
        for k in range(1, PIECES):
            z_copy(k).start()

    for bits in (4, 6):
        hand_x(bits)
        hand_sib(bits)

    @pl.when(inner)
    def _():
        for k in range(2, EARLY_X):
            x_copy(k).start()

    z_copy(0).wait_recv()
    d_copy(0).start()
    wi_copy.wait_recv()
    start(wi_mine, wi_mine, yn, "WIY")
    start(wi_mine, wi_mine, sib, "WIS1")
    for bits in (1, 3, 5, 7):
        arrive(bits, f"F{bits}")
        hand_sib(bits)
    remote(wi_other, wi_other, yn, "WIY").wait_recv()
    start(wi_other, wi_other, sib, "WIS2")
    @pl.when(inner)
    def _():
        for k in range(1, EARLY_D):
            z_copy(k).wait_recv()
            d_copy(k).start()

    for k in range(EARLY_X, LATE_X):
        x_copy(k).start()
    hand_wo(0)
    remote(bin_ref, PB, z2, "BZ").wait_recv()
    remote(
        wi_ref, WI.at[0, pl.ds(aligned((1 - core) * dvh, dvh), dvh)], sib, "WIS0"
    ).wait_recv()
    for name, y in (("WIS1", img), ("WIS2", 1 - img)):
        piece = WI.at[1, pl.ds(aligned((1 - core) * dvh + y * dvq, dvq), dvq)]
        remote(piece, piece, sib, name).wait_recv()
    for bits in range(8):
        block = feat_block(bits, 1 - core)
        remote(block, block, sib, f"S{bits}").wait_recv()
    for copy in (locals_[1], locals_[3]):
        copy.wait()

    @pl.loop(0, stride)
    def _(t):
        block = inside + t % 2 - 2 * (t % 2) * (inside % 2)
        block = block + 2 * (t // 2) - 4 * (t // 2) * ((block // 2) % 2)
        first = block * rows + core * tile
        place = first + lax.broadcasted_iota(jnp.int32, (tile, 1), 0)
        row = lookup(place)
        kept = jnp.where(row >= 0, 1.0, 0.0).astype(F32)
        wanted = lax.broadcasted_iota(jnp.int32, (tile, tokens), 1) == row
        chosen = jnp.where(wanted, 1.0, 0.0).astype(BF16)
        values = jnp.dot(chosen, F[...], preferred_element_type=F32)
        here = pl.ds(aligned(t * tile, tile), tile)
        V[here] = values.astype(BF16)
        mean = jnp.mean(values, axis=1, keepdims=True)
        centred = values - mean
        rstd = lax.rsqrt(jnp.mean(centred * centred, axis=1, keepdims=True) + 1e-05)
        MEAN[here] = mean
        RSTD[here] = rstd
        scaled = centred * rstd * gain_ref[...] + bias_ref[...]
        normed_in = scaled.astype(BF16)
        NT[:, here] = scaled.T.astype(BF16)
        for g in range(samples):
            shift_row = bin_ref[...] if g == 0 else PB[...]
            preact = jnp.dot(normed_in, WI[g], preferred_element_type=F32) + shift_row
            activ, slope = gelu_parts(preact)
            columns = pl.ds(g * hb, hb)
            SL[here, columns] = slope * kept
            HT[columns, pl.ds(aligned(t * rows + core * tile, tile), tile)] = (
                (activ * kept).T.astype(BF16)
            )
        ht_copy(t).start()

        @pl.when(t == 2)
        def _():
            @pl.when(outer)
            def _():
                hand_wo(1)

    @pl.when(outer)
    def _():
        for k in range(1, EARLY_D):
            z_copy(k).wait_recv()
            d_copy(k).start()

    for t in range(stride):
        remote(ht_piece(t, 1 - core), ht_piece(t, 1 - core), sib, "HT", k=t, count=stride).wait_recv()
    def y_copy(k):
        columns = pl.ds(aligned(k * ck, ck), ck)
        return remote(YS.at[:, columns], YR.at[:, columns], yn, "YK", k=k, count=PIECES)

    def zk_copy(k):
        columns = pl.ds(aligned(k * ck, ck), ck)
        return remote(ZS.at[:, columns], ZR.at[:, columns], z2, "ZK", k=k, count=PIECES)

    def weight_grad(k):
        columns = pl.ds(aligned(k * ck, ck), ck)
        piece = L[:, columns]
        for g in range(samples):
            mine = pl.ds(aligned(g * hb + img * hh, hh), hh)
            other = pl.ds(aligned(g * hb + (1 - img) * hh, hh), hh)
            sent = jnp.dot(HT[other], piece, preferred_element_type=F32)
            YS[pl.ds(g * hh, hh), columns] = sent.astype(BF16)
            kept = jnp.dot(HT[mine], piece, preferred_element_type=F32)
            if g == 0:
                wo_out[:, columns] = kept
            else:
                GP[:, columns] = kept
        y_copy(k).start()

    def hidden_part(k, s, g, low, size):
        columns = pl.ds(aligned(k * ck, ck), ck)
        HP[s, :, pl.ds(aligned(g * hb + low, hh), size)] += lax.dot_general(
            L[pl.ds(aligned(s * rows, rows), rows), columns],
            W[g, pl.ds(aligned(low, hh), size), columns],
            (((1,), (1,)), ((), ())),
            preferred_element_type=F32,
        )

    def half_rows(c):
        return pl.ds(aligned(c * tile, tile), tile)

    def exchange(s):
        PG[pl.ds(aligned(s * tile, tile), tile)] = HP[s, half_rows(1 - core)].astype(BF16)
        hr_copy(s).start()

    def preact_grad(s):
        copy = hr_copy(s)
        copy.wait()
        here = pl.ds(s * tile, tile)
        grad = HP[s, half_rows(core)] + HR[here].astype(F32)
        rounded = (grad * SL[here]).astype(BF16)
        PG[here] = rounded
        ACC[pl.ds(0, 1)] += jnp.sum(rounded.astype(F32), axis=0, keepdims=True)

    def over_img(k):
        columns = pl.ds(aligned(k * ck, ck), ck)
        y_copy(k).wait_recv()
        wo_out[:, columns] += YR[pl.ds(0, hh), columns].astype(F32)
        both = GP[:, columns] + YR[pl.ds(hh, hh), columns].astype(F32)
        ZS[:, columns] = both.astype(BF16)
        zk_copy(k).start()

    def over_samples(k):
        columns = pl.ds(aligned(k * ck, ck), ck)
        zk_copy(k).wait_recv()
        wo_out[:, columns] += ZR[:, columns].astype(F32)

    ACC[...] = jnp.zeros(ACC.shape, F32)

    last = stride - 1

    def hidden_parts(k, s):
        hidden_part(k, s, 0, 0, hb)
        for n in range(LATE_MINE, PIECES):

            @pl.when(k == n)
            def _():
                for late, step, y in ((LATE_MINE, 2, img), (LATE, 2, 1 - img)):
                    low = min(step * (n - late), n)
                    high = min(step * (n - late) + step, n + 1)
                    if n >= late:

                        @pl.loop(low, high)
                        def _(j):
                            for g in range(1, samples):
                                hidden_part(j, s, g, y * hh, hh)

    @pl.loop(0, PIECES)
    def _(k):
        x_copy(k).wait_recv()

        @pl.when(k == LATE)
        def _():
            for n in range(2):
                piece = W.at[1, wo_piece(1 - img, n)]
                remote(piece, piece, yn, f"WY{n}").wait_recv()

        @pl.loop(0, last)
        def _(s):
            hidden_parts(k, s)

            @pl.when(k == PIECES - 1)
            def _():
                exchange(s)

        d_copy(k).wait_recv()
        weight_grad(k)

        @pl.when(k >= 1)
        def _():
            over_img(k - 1)

        hidden_parts(k, last)

        @pl.when(k == PIECES - 1)
        def _():
            exchange(last)

        @pl.when(k + EARLY_D < PIECES)
        def _():
            z_copy(k + EARLY_D).wait_recv()
            d_copy(k + EARLY_D).start()

        @pl.when(k == 2)
        def _():
            @pl.when(inner)
            def _():
                hand_wo(1)

        for n in range(LATE_X, PIECES):

            @pl.when(k == n - LATE_X)
            def _():
                x_copy(n).start()


    for s in range(last):
        preact_grad(s)
    preact_grad(last)

    def first_grad(block):
        lines = pl.ds(aligned(block * dvq, dvq), dvq)
        return jnp.dot(NT[lines], PG[...], preferred_element_type=F32)

    mine_rows = pl.ds(aligned(img * dvq, dvq), dvq)
    other_rows = pl.ds(aligned((1 - img) * dvq, dvq), dvq)
    own_cols = pl.ds(0, hb)
    far_cols = [pl.ds(hb + n * (hb // 2), hb // 2) for n in range(2)]

    def send_img():
        WYS[...] = HP[0, other_rows].astype(BF16)
        for n in range(2):
            start(WYS.at[:, far_cols[n]], WYR.at[:, far_cols[n]], yn, f"WYF{n}")
        start(WYS.at[:, own_cols], WYR.at[:, own_cols], yn, "WYO")

    def kept_rows(y):
        return pl.ds(aligned(y * dvq, dvq), dvq)

    def wg_copy(n, y):
        return remote(WS.at[y], WR.at[y], sib, f"WG{n}")

    for n, y in enumerate((1 - img, img)):
        WS[y] = first_grad(2 * y + 1 - core).astype(BF16)
        wg_copy(n, y).start()
        HP[0, kept_rows(y)] = first_grad(2 * y + core)
        if n == 0:
            wg_copy(n, y).wait_recv()
            HP[0, kept_rows(y)] += WR[y].astype(F32)
            send_img()
    wg_copy(1, img).wait_recv()
    over_img(PIECES - 1)
    def over_far(n):
        local = pl.ds(n * (hb // 2), hb // 2)
        columns = far_cols[n]
        remote(WYS.at[:, columns], WYR.at[:, columns], yn, f"WYF{n}").wait_recv()
        total = HP[0, mine_rows, columns] + WR[img, :, columns].astype(F32)
        WZS[:, local] = (total + WYR[:, columns].astype(F32)).astype(BF16)
        start(WZS.at[:, local], WZR.at[:, local], z2, f"WZS{n}")

    over_far(0)

    @pl.loop(0, part // tile)
    def _(t):
        here = pl.ds(aligned(t * tile, tile), tile)
        grad = jnp.zeros((tile, dv), F32)
        for g in range(samples):
            grad = grad + lax.dot_general(
                PG[here, pl.ds(g * hb, hb)],
                WI[g],
                (((1,), (1,)), ((), ())),
                preferred_element_type=F32,
            )
        normed = (V[here].astype(F32) - MEAN[here]) * RSTD[here]
        ACC[pl.ds(1, 1)] += jnp.sum(grad * normed, axis=0, keepdims=True)
        ACC[pl.ds(2, 1)] += jnp.sum(grad, axis=0, keepdims=True)

    put_small(gain_row, ACC[pl.ds(1, 1)][:, :dv])
    put_small(bias_row, ACC[pl.ds(2, 1)][:, :dv])
    sums = ACC[pl.ds(0, 1)]
    for g in range(samples):
        put_small(
            b_in_row + flip(seq, 4 * g) * (hb // lanes), sums[:, g * hb : (g + 1) * hb]
        )

    def small_start(n, target, place=None):
        place = n if place is None else place
        start(SV.at[n], AR.at[place], target, f"AR{place}")

    def small_wait(n):
        remote(SV.at[0], AR.at[n], sib, f"AR{n}").wait_recv()

    small_start(0, sib)
    over_far(1)
    small_wait(0)
    SV[1] = SV[0] + AR[0]
    small_start(1, xn)
    small_wait(1)
    SV[2] = SV[1] + AR[1]
    small_start(2, yn)
    small_wait(2)
    SV[3] = SV[2] + AR[2]
    for n, target in enumerate((z1, z2, z3)):
        small_start(3, target, 3 + n)
    remote(WYS.at[:, own_cols], WYR.at[:, own_cols], yn, "WYO").wait_recv()
    wi_out[...] = (HP[0, mine_rows, own_cols] + WR[img, :, own_cols].astype(F32)
                   + WYR[:, own_cols].astype(F32))
    def wo_store(k):
        columns = pl.ds(aligned(k * ck, ck), ck)
        return pltpu.make_async_copy(
            wo_out.at[:, columns], wo_hbm.at[:, columns], out_sem.at[k]
        )

    @pl.loop(0, PIECES)
    def _(k):
        over_samples(k)
        wo_store(k).start()

    for n in range(2):
        local = pl.ds(n * (hb // 2), hb // 2)
        remote(WZS.at[:, local], WZR.at[:, local], z2, f"WZS{n}").wait_recv()
        wi_out[:, local] += WZR[:, local].astype(F32)
    for n in range(3, 6):
        small_wait(n)
    small_out[...] = (SV[3] + AR[3]) + (AR[4] + AR[5])
    stores = [pltpu.make_async_copy(wi_out, wi_hbm, out_sem.at[PIECES])]
    row = 0
    for n, ref in enumerate((gain_hbm, bias_hbm, b_in_hbm, b_out_hbm)):
        piece = small_out.at[pl.ds(row, ref.shape[0])]
        stores.append(pltpu.make_async_copy(piece, ref, out_sem.at[PIECES + 1 + n]))
        row += ref.shape[0]
    for copy in stores:
        copy.start()
    for copy in started:
        copy.wait_send()

    @pl.when(inner)
    def _():
        for copy in (cut_own, cut_pair, back_near, back_far):
            copy.wait_send()

    for n in range(2):
        piece = W.at[1, wo_piece(img, n)]
        remote(piece, piece, yn, f"WY{n}").wait_send()
    for t in range(stride):
        ht_copy(t).wait_send()
    for copy in (wi_copy, *wo_copies, wg_copy(0, 1 - img), wg_copy(1, img)):
        copy.wait_send()

    @pl.loop(0, PIECES)
    def _(k):
        for copy in (x_copy, z_copy, d_copy, y_copy, zk_copy):
            copy(k).wait_send()

    @pl.loop(0, PIECES)
    def _(k):
        wo_store(k).wait()

    for copy in stores:
        copy.wait()


def finish_body(ins, outs, held, sems):
    copies = []
    for n, (source, place) in enumerate(zip(ins, held)):
        copy = pltpu.make_async_copy(source, place, sems.at[0, n])
        copy.start()
        copies.append(copy)
    later = []
    for n, (place, target) in enumerate(zip(held, outs)):
        copies[n].wait()
        copy = pltpu.make_async_copy(place, target, sems.at[1, n])
        copy.start()
        later.append(copy)
    for copy in later:
        copy.wait()


def finish(values):
    count = len(values)
    hbm = pl.BlockSpec(memory_space=pl.ANY)

    def body(*refs):
        finish_body(refs[:count], refs[count : 2 * count], refs[2 * count : -1], refs[-1])

    return pl.pallas_call(
        body,
        out_shape=[jax.ShapeDtypeStruct(v.shape, v.dtype) for v in values],
        in_specs=[hbm] * count,
        out_specs=[hbm] * count,
        scratch_shapes=[pltpu.VMEM(v.shape, v.dtype) for v in values]
        + [pltpu.SemaphoreType.DMA((2, count))],
    )(*values)


def per_device_kernel(
    vision_feats, ln_gain, ln_bias, w_in, b_in, w_out, lm_grad, image_counts, token_pos
):
    seq_count = lax.axis_size("seq")
    _, rows, half = lm_grad.shape
    hb = w_out.shape[0]
    dv = ln_gain.shape[0]
    frows = vision_feats.shape[1]
    tokens = token_pos.shape[1]
    samples = image_counts.shape[1]
    stride = seq_count // samples
    span = stride * rows
    part = span // 2
    hid = samples * hb
    images = tokens // PATCH
    lanes = 128
    small = (2 * dv + seq_count * hb + 2 * half) // lanes
    dims = (rows, half, hb, dv, frows, tokens, seq_count, samples, images)
    vmem = pl.BlockSpec(memory_space=pltpu.VMEM)
    smem = pl.BlockSpec(memory_space=pltpu.SMEM)
    hbm = pl.BlockSpec(memory_space=pl.ANY)
    wo, wi, *sums = pl.pallas_call(
        functools.partial(kernel_body, dims),
        out_shape=(
            jax.ShapeDtypeStruct((hb // 2, half), F32),
            jax.ShapeDtypeStruct((dv // 4, hb), F32),
            jax.ShapeDtypeStruct((dv // lanes, lanes), F32),
            jax.ShapeDtypeStruct((dv // lanes, lanes), F32),
            jax.ShapeDtypeStruct((seq_count * hb // lanes, lanes), F32),
            jax.ShapeDtypeStruct((2 * half // lanes, lanes), F32),
        ),
        in_specs=[smem, smem, hbm, vmem, vmem, hbm, vmem, hbm, hbm],
        out_specs=[hbm] * 6,
        scratch_shapes=[
            pltpu.VMEM((span, half), BF16),
            pltpu.VMEM((samples, hb, half), BF16),
            pltpu.VMEM((samples, dv, hb), BF16),
            pltpu.VMEM((tokens, dv), BF16),
            pltpu.VMEM((dv, part), BF16),
            pltpu.VMEM((part, dv), BF16),
            pltpu.VMEM((part, 1), F32),
            pltpu.VMEM((part, 1), F32),
            pltpu.VMEM((part, hid), F32),
            pltpu.VMEM((hid, span), BF16),
            pltpu.VMEM((stride, rows, hid), F32),
            pltpu.VMEM((part, hid), BF16),
            pltpu.VMEM((part, hid), BF16),
            pltpu.VMEM((hb, half), BF16),
            pltpu.VMEM((hb, half), BF16),
            pltpu.VMEM((hb // 2, half), BF16),
            pltpu.VMEM((hb // 2, half), BF16),
            pltpu.VMEM((hb // 2, half), F32),
            pltpu.VMEM((2, dv // 4, hid), BF16),
            pltpu.VMEM((2, dv // 4, hid), BF16),
            pltpu.VMEM((dv // 4, hid), BF16),
            pltpu.VMEM((dv // 4, hid), BF16),
            pltpu.VMEM((dv // 4, hb), BF16),
            pltpu.VMEM((dv // 4, hb), BF16),
            pltpu.VMEM((1, hb), F32),
            pltpu.VMEM((8, max(hid, dv)), F32),
            pltpu.VMEM((4, small, lanes), F32),
            pltpu.VMEM((6, small, lanes), F32),
            pltpu.VMEM((hb // 2, half), F32),
            pltpu.VMEM((dv // 4, hb), F32),
            pltpu.VMEM((small, lanes), F32),
            pltpu.SemaphoreType.DMA((PIECES + 5,)),
            pltpu.SemaphoreType.DMA((96,)),
            pltpu.SemaphoreType.DMA((96,)),
            pltpu.SemaphoreType.DMA((4,)),
        ],
        compiler_params=pltpu.CompilerParams(
            collective_id=0, has_side_effects=True, vmem_limit_bytes=67043328
        ),
    )(
        image_counts,
        token_pos,
        vision_feats[0],
        ln_gain[None],
        ln_bias[None],
        w_in,
        b_in[None],
        w_out,
        lm_grad[0],
    )
    wo, wi, *sums = finish((wo, wi, *sums))
    gain_grad, bias_grad, b_in_grad, b_out_grad = (value.reshape(-1) for value in sums)
    return (wi, b_in_grad, wo, b_out_grad, gain_grad, bias_grad)


def dispatch(mesh, *args):
    sizes = (mesh.shape["seq"], mesh.shape["img"], mesh.shape["fsdp"])
    if sizes == (8, 2, 2) and args[7].shape[1] == 2:
        return per_device_kernel(*args)
    return per_device(*args)


def solution(mesh):
    return jax.shard_map(
        functools.partial(dispatch, mesh),
        mesh=mesh,
        in_specs=(
            P("img", ("seq", "fsdp"), None),
            P(),
            P(),
            P("fsdp", "seq"),
            P("seq"),
            P("seq", "fsdp"),
            P("img", "seq", "fsdp"),
            P("img", None),
            P("img", None),
        ),
        out_specs=(
            P(("img", "fsdp"), "seq"),
            P(),
            P(("seq", "img"), "fsdp"),
            P(),
            P(),
            P(),
        ),
        check_vma=False,
    )
```

```python
import functools

import jax
import jax.numpy as jnp
from jax import lax
from jax.experimental import pallas as pl
from jax.experimental.pallas import tpu as pltpu
from jax.sharding import PartitionSpec as P

PATCH = 576
CHUNKS = 2
PIECES = 8
EARLY_X = 4
EARLY_D = 2
LATE_X = 6
LATE_MINE = 2
LATE = 3
BF16 = jnp.bfloat16
F32 = jnp.float32


def gelu_parts(preact):
    cumul = 0.5 * (1.0 + lax.erf(preact * 0.7071067811865476))
    density = jnp.exp(-0.5 * preact * preact) * 0.3989422804014327
    return (preact * cumul, cumul + preact * density)


def contract(left, right, left_dim, right_dim):
    return lax.dot_general(
        left, right, (((left_dim,), (right_dim,)), ((), ())), preferred_element_type=jnp.float32
    )


def shift(value, axis, amount):
    count = lax.axis_size(axis)
    return lax.ppermute(value, axis, [(i, (i + amount) % count) for i in range(count)])


def flip(value, bit):
    count = lax.axis_size("seq")
    return lax.ppermute(value, "seq", [(i, i ^ bit) for i in range(count)])


def pick(value, index, axis):
    return lax.dynamic_index_in_dim(value, index, axis=axis, keepdims=False)


def scatter_sum(value, axis):
    count = lax.axis_size(axis)
    index = lax.axis_index(axis)
    if count > 2:
        return lax.psum_scatter(value, axis, scatter_dimension=0, tiled=False)
    if count == 1:
        return value[0]
    sent = pick(value, 1 - index, 0).astype(jnp.bfloat16)
    return pick(value, index, 0) + shift(sent, axis, 1).astype(jnp.float32)


def sample_sum(value, stride, after):
    total, _ = lax.optimization_barrier((value[0], after))
    for k in range(1, value.shape[0]):
        moved = shift(value[k].astype(jnp.bfloat16), "seq", -k * stride)
        total = total + moved.astype(jnp.float32)
    return total


def per_device(vision_feats, ln_gain, ln_bias, w_in, b_in, w_out, lm_grad, image_counts, token_pos):
    seq_count = lax.axis_size("seq")
    seq_index = lax.axis_index("seq")
    img_count = lax.axis_size("img")
    fsdp_count = lax.axis_size("fsdp")
    fsdp_index = lax.axis_index("fsdp")
    lm_block = lm_grad[0]
    block_rows, half_width = lm_block.shape
    counts = image_counts[0]
    samples = counts.shape[0]
    stride = seq_count // samples
    sample_len = stride * block_rows
    own_sample = seq_index // stride
    positions = token_pos[0]
    row_count = positions.shape[0]
    images = row_count // PATCH
    starts = positions.reshape(images, PATCH)[:, 0]
    bounds = jnp.cumsum(counts)
    image_index = jnp.arange(images, dtype=jnp.int32)
    image_sample = jnp.sum((image_index[:, None] >= bounds[None, :]).astype(jnp.int32), axis=1)
    in_sample = image_sample == own_sample

    def lookup(place):
        offset = place[:, None] - starts[None, :]
        match = in_sample[None, :] & (offset >= 0) & (offset < PATCH)
        row = jnp.sum(jnp.where(match, offset + image_index[None, :] * PATCH, 0), axis=1)
        return row, jnp.any(match, axis=1)

    own_place = (seq_index % stride) * block_rows + jnp.arange(block_rows, dtype=jnp.int32)
    own_mask = lookup(own_place)[1].astype(jnp.bfloat16)
    out_bias_half = jnp.dot(own_mask[None, :], lm_block, preferred_element_type=jnp.float32)[0]
    out_bias_whole = lax.dynamic_update_slice_in_dim(
        jnp.zeros((half_width * fsdp_count,), jnp.float32),
        out_bias_half,
        fsdp_index * half_width,
        0,
    )

    feats = lax.all_gather(vision_feats[0], ("seq", "fsdp"), axis=0, tiled=True)

    in_blocks = [w_in] + [shift(w_in, "seq", k * stride) for k in range(1, samples)]
    in_bias = jnp.concatenate([b_in] + [shift(b_in, "seq", k * stride) for k in range(1, samples)])
    w_in_half = jnp.concatenate(in_blocks, axis=1)
    w_in_full = lax.all_gather(w_in_half, "fsdp", axis=0, tiled=True)
    w_out_later, _ = lax.optimization_barrier((w_out, w_in_half))
    w_out_full = jnp.concatenate(
        [w_out] + [shift(w_out_later, "seq", k * stride) for k in range(1, samples)], axis=0
    )
    hid = in_bias.shape[0]
    block_hid = hid // samples

    groups = [[s * stride + i for i in range(stride)] for s in range(samples)]
    width = half_width // CHUNKS
    slices = [lm_block[:, c * width : (c + 1) * width] for c in range(CHUNKS)]
    crossed = stride == 4
    if crossed:
        pieces = []
        for piece in slices:
            far = flip(piece, 2)
            near = flip(piece, 1)
            pieces.append(jnp.concatenate([piece, near, far, flip(far, 1)], axis=0))
    else:
        pieces = [
            lax.all_gather(piece, "seq", axis=0, tiled=True, axis_index_groups=groups)
            for piece in slices
        ]
    b_out_grad = lax.psum(out_bias_whole, ("seq", "img", "fsdp"))
    feats, b_out_grad = lax.optimization_barrier((feats, b_out_grad))

    part_len = sample_len // fsdp_count
    place = fsdp_index * part_len + jnp.arange(part_len, dtype=jnp.int32)
    if crossed:
        block = place // block_rows
        place = (block ^ (seq_index % stride)) * block_rows + place % block_rows
    row, mask = lookup(place)
    values = feats.at[row].get(mode="promise_in_bounds").astype(jnp.float32)
    row_mean = jnp.mean(values, axis=1, keepdims=True)
    centred = values - row_mean
    row_var = jnp.mean(centred * centred, axis=1, keepdims=True)
    normed = centred * lax.rsqrt(row_var + 1e-05)
    normed_in = (normed * ln_gain + ln_bias).astype(jnp.bfloat16)
    preact = jnp.dot(normed_in, w_in_full, preferred_element_type=jnp.float32) + in_bias
    activ, slope = gelu_parts(preact)
    hidden = jnp.where(mask[:, None], activ, 0.0).astype(jnp.bfloat16)
    slope = jnp.where(mask[:, None], slope, 0.0)
    if fsdp_count == 2:
        other = shift(hidden, "fsdp", 1)
        first = fsdp_index == 0
        hidden_full = jnp.concatenate(
            [jnp.where(first, hidden, other), jnp.where(first, other, hidden)], axis=0
        )
    else:
        hidden_full = lax.all_gather(hidden, "fsdp", axis=0, tiled=True)

    w_out_grads = []
    hidden_part = 0.0
    hidden_full, pieces[0] = lax.optimization_barrier((hidden_full, pieces[0]))
    for c in range(CHUNKS):
        piece = pieces[c]
        part = contract(hidden_full, piece, 0, 0)
        part = part.reshape(samples, img_count, block_hid // img_count, width)
        part = scatter_sum(part.transpose(1, 0, 2, 3), "img")
        w_out_grads.append(part)
        hidden_part = hidden_part + contract(
            piece, w_out_full[:, c * width : (c + 1) * width], 1, 1
        )

    hidden_grad = scatter_sum(hidden_part.reshape(fsdp_count, part_len, hid), "fsdp")
    preact_grad = (hidden_grad * slope).astype(jnp.bfloat16)
    in_part = contract(normed_in, preact_grad, 0, 0)
    in_part = in_part.reshape(img_count, fsdp_count, -1, samples, block_hid)
    in_part = scatter_sum(in_part.transpose(1, 0, 2, 3, 4), "fsdp")
    in_part = scatter_sum(in_part, "img")

    b_in_part = jnp.sum(preact_grad, axis=0, dtype=jnp.float32)
    normed_grad = contract(preact_grad, w_in_full, 1, 1)
    gain_part = jnp.sum(normed_grad * normed, axis=0)
    bias_part = jnp.sum(normed_grad, axis=0)
    hidden_bias = jnp.zeros((seq_count, block_hid), jnp.float32)
    for k in range(samples):
        owner = (seq_index - k * stride + seq_count) % seq_count
        hidden_bias = lax.dynamic_update_slice(
            hidden_bias, b_in_part[None, k * block_hid : (k + 1) * block_hid], (owner, 0)
        )
    gain_grad, bias_grad, b_in_grad = lax.psum(
        (gain_part, bias_part, hidden_bias.reshape(-1)), ("seq", "img", "fsdp")
    )
    w_in_grad = sample_sum(in_part.transpose(1, 0, 2), stride, gain_grad)
    w_out_grad = jnp.concatenate(
        [sample_sum(part, stride, gain_grad) for part in w_out_grads], axis=1
    )
    return (w_in_grad, b_in_grad, w_out_grad, b_out_grad, gain_grad, bias_grad)


def kernel_body(
    dims,
    counts_ref,
    pos_ref,
    feats_ref,
    gain_ref,
    bias_ref,
    wi_ref,
    bin_ref,
    wo_ref,
    lm_ref,
    wo_hbm,
    wi_hbm,
    gain_hbm,
    bias_hbm,
    b_in_hbm,
    b_out_hbm,
    L,
    W,
    WI,
    F,
    NT,
    V,
    MEAN,
    RSTD,
    SL,
    HT,
    HP,
    PG,
    HR,
    YS,
    YR,
    ZS,
    ZR,
    GP,
    WS,
    WR,
    WYS,
    WYR,
    WZS,
    WZR,
    PB,
    ACC,
    SV,
    AR,
    wo_out,
    wi_out,
    small_out,
    out_sem,
    send_sem,
    recv_sem,
    local_sem,
):
    rows, half, hb, dv, frows, tokens, seq_count, samples, images = dims
    stride = seq_count // samples
    span = stride * rows
    part = span // 2
    hid = samples * hb
    hh = hb // 2
    dvh = dv // 2
    dvq = dv // 4
    ck = half // PIECES
    seq = lax.axis_index("seq")
    img = lax.axis_index("img")
    core = lax.axis_index("fsdp")

    def flip(value, bits):
        for bit in (1, 2, 4):
            if bits & bit:
                value = value + bit - 2 * bit * ((value // bit) % 2)
        return value

    def device(bits=0, y=0, c=0):
        return (
            flip(seq, bits),
            1 - img if y else img,
            1 - core if c else core,
        )

    z1 = device(2)
    z2 = device(4)
    z3 = device(6)
    xn = device(1)
    yn = device(y=1)
    sib = device(c=1)

    names = {}

    def slot(name, count=1):
        if name not in names:
            names[name] = sum(c for _, c in names.values()), count
        return names[name][0]

    def remote(src, dst, target, recv, send=None, k=0, count=1):
        return pltpu.make_async_remote_copy(
            src_ref=src,
            dst_ref=dst,
            send_sem=send_sem.at[slot(send or recv, count) + k],
            recv_sem=recv_sem.at[slot(recv, count) + k],
            device_id=target,
            device_id_type=pl.DeviceIdType.MESH,
        )

    started = []

    def start(*args, **kwargs):
        copy = remote(*args, **kwargs)
        copy.start()
        started.append(copy)

    def aligned(value, unit):
        return pl.multiple_of(value, unit)

    def feat_block(bits, c):
        return F.at[pl.ds(aligned((flip(seq, bits) * 2 + c) * frows, 16), frows)]

    inside = seq % stride
    sample = seq // stride
    bounds = [counts_ref[0, 0] * 0]
    for s in range(samples):
        bounds.append(bounds[-1] + counts_ref[0, s])
    low = bounds[0]
    high = bounds[1]
    for s in range(1, samples):
        low = jnp.where(sample == s, bounds[s], low)
        high = jnp.where(sample == s, bounds[s + 1], high)
    begins = []
    for n in range(images):
        here = jnp.where(n >= low, jnp.where(n < high, 1, 0), 0)
        begins.append(jnp.where(here == 1, pos_ref[0, n * PATCH], 2 * span))

    def lookup(place):
        row = jnp.full(place.shape, -1, jnp.int32)
        for n in range(images):
            offset = place - begins[n]
            match = jnp.logical_and(offset >= 0, offset < PATCH)
            row = jnp.where(match, offset + n * PATCH, row)
        return row

    lanes = SV.shape[2]
    gain_row, bias_row = 0, dv // lanes
    b_in_row = 2 * (dv // lanes)
    b_out_row = b_in_row + seq_count * (hb // lanes)

    def put_small(row, value):
        for m in range(value.shape[1] // lanes):
            SV[0, pl.ds(row + m, 1)] = value[:, m * lanes : (m + 1) * lanes]

    def own_sums():
        place = inside * rows + lax.broadcasted_iota(jnp.int32, (rows, 1), 0)
        own_kept = jnp.where(lookup(place) >= 0, 1.0, 0.0).astype(F32)
        for m in range(half // hb):
            block = L[pl.ds(0, rows), pl.ds(m * hb, hb)].astype(F32) * own_kept
            total = jnp.sum(block, axis=0, keepdims=True)
            put_small(b_out_row + core * (half // lanes) + m * (hb // lanes), total)

    barrier = pltpu.get_barrier_semaphore()
    for target in (z1, z2, z3, xn, yn, sib):
        pl.semaphore_signal(
            barrier, inc=1, device_id=target, device_id_type=pl.DeviceIdType.MESH
        )

    locals_ = [
        pltpu.make_async_copy(feats_ref, feat_block(0, core), local_sem.at[0]),
        pltpu.make_async_copy(
            wi_ref, WI.at[0, pl.ds(aligned(core * dvh, dvh), dvh)], local_sem.at[1]
        ),
        pltpu.make_async_copy(lm_ref, L.at[pl.ds(0, rows)], local_sem.at[2]),
        pltpu.make_async_copy(wo_ref, W.at[0], local_sem.at[3]),
    ]
    for copy in locals_:
        copy.start()
    pl.semaphore_wait(barrier, 6)

    def lm_piece(k, index):
        columns = pl.ds(aligned(k * ck, ck), ck)
        return L.at[pl.ds(index * rows, rows), columns]

    def lm_own(k):
        return lm_ref.at[:, pl.ds(aligned(k * ck, ck), ck)]

    def x_copy(k):
        return remote(lm_own(k), lm_piece(k, 1), xn, "X", k=k, count=PIECES)

    def z_copy(k):
        return remote(lm_own(k), lm_piece(k, 2), z1, "Z", k=k, count=PIECES)

    def d_copy(k):
        return remote(lm_piece(k, 2), lm_piece(k, 3), xn, "D", k=k, count=PIECES)

    zseq = seq // 2
    inner = (zseq + 1) // 2 == 1

    def ht_copy(t):
        return remote(ht_piece(t, core), ht_piece(t, core), sib, "HT", k=t, count=stride)

    def hr_copy(s):
        here = pl.ds(aligned(s * tile, tile), tile)
        return remote(PG.at[here], HR.at[here], sib, "HR", k=s, count=stride)
    wi_rows = pl.ds(aligned(img * dvq, dvq), dvq)
    wi_mine = WI.at[1, pl.ds(aligned(core * dvh + img * dvq, dvq), dvq)]
    wi_other = WI.at[1, pl.ds(aligned(core * dvh + (1 - img) * dvq, dvq), dvq)]
    quarter = hh // 2

    def wo_piece(y, n):
        return pl.ds(aligned(y * hh + n * quarter, quarter), quarter)

    def hand_wo(n):
        piece = W.at[1, wo_piece(img, n)]
        remote(piece, piece, z2, f"WZ{n}").wait_recv()
        remote(piece, piece, yn, f"WY{n}").start()

    def ht_piece(s, c):
        return HT.at[:, pl.ds(aligned(s * rows + c * tile, tile), tile)]

    tile = rows // 2

    start(feats_ref, feat_block(0, core), z1, "F2")
    start(bin_ref, PB, z2, "BZ")
    wi_copy = remote(wi_ref.at[wi_rows], wi_mine, z2, "WIZ")
    wo_copies = [
        remote(wo_ref.at[wo_piece(img, n)], W.at[1, wo_piece(img, n)], z2, f"WZ{n}")
        for n in range(2)
    ]
    outer = 1 - (zseq + 1) // 2 % 2 == 1

    @pl.when(inner)
    def _():
        wi_copy.start()

    z_copy(0).start()

    @pl.when(outer)
    def _():
        for k in range(1, 3):
            z_copy(k).start()
        wi_copy.start()
        wo_copies[0].start()
        for k in range(3, PIECES - 1):
            z_copy(k).start()
        wo_copies[1].start()
        z_copy(PIECES - 1).start()

    start(feats_ref, feat_block(0, core), xn, "F1")
    x_copy(0).start()
    start(feats_ref, feat_block(0, core), sib, "S0")
    start(wi_ref, WI.at[0, pl.ds(aligned(core * dvh, dvh), dvh)], sib, "WIS0")

    def arrive(bits, name):
        remote(feats_ref, feat_block(bits, core), xn, name).wait_recv()

    def hand_x(bits):
        block = feat_block(bits, core)
        start(block, block, xn, f"F{bits + 1}")

    def hand_sib(bits):
        block = feat_block(bits, core)
        start(block, block, sib, f"S{bits}")

    arrive(2, "F2")
    locals_[0].wait()
    own_block, pair_block = feat_block(0, core), feat_block(2, core)
    far_block, near_block = feat_block(4, core), feat_block(6, core)
    cut_own = remote(own_block, own_block, z3, "F6", send="C0")
    cut_pair = remote(pair_block, pair_block, z3, "F4", send="C1")
    back_near = remote(near_block, near_block, z1, "F4", send="C2")
    back_far = remote(far_block, far_block, z1, "F6", send="C3")

    @pl.when(inner)
    def _():
        cut_own.start()
        cut_pair.start()

    hand_x(2)
    hand_sib(2)
    x_copy(1).start()

    @pl.when(outer)
    def _():
        for k in range(2, EARLY_X):
            x_copy(k).start()

    HP[...] = jnp.zeros(HP.shape, F32)
    ACC[...] = jnp.zeros(ACC.shape, F32)
    SV[0] = jnp.zeros(SV.shape[1:], F32)
    locals_[2].wait()
    own_sums()
    arrive(4, "F4")
    arrive(6, "F6")

    @pl.when(inner)
    def _():
        back_near.start()
        back_far.start()
        for copy in wo_copies:
            copy.start()
        for k in range(1, PIECES):
            z_copy(k).start()

    for bits in (4, 6):
        hand_x(bits)
        hand_sib(bits)

    @pl.when(inner)
    def _():
        for k in range(2, EARLY_X):
            x_copy(k).start()

    z_copy(0).wait_recv()
    d_copy(0).start()
    wi_copy.wait_recv()
    start(wi_mine, wi_mine, yn, "WIY")
    start(wi_mine, wi_mine, sib, "WIS1")
    for bits in (1, 3, 5, 7):
        arrive(bits, f"F{bits}")
        hand_sib(bits)
    remote(wi_other, wi_other, yn, "WIY").wait_recv()
    start(wi_other, wi_other, sib, "WIS2")
    @pl.when(inner)
    def _():
        for k in range(1, EARLY_D):
            z_copy(k).wait_recv()
            d_copy(k).start()

    for k in range(EARLY_X, LATE_X):
        x_copy(k).start()
    hand_wo(0)
    remote(bin_ref, PB, z2, "BZ").wait_recv()
    remote(
        wi_ref, WI.at[0, pl.ds(aligned((1 - core) * dvh, dvh), dvh)], sib, "WIS0"
    ).wait_recv()
    for name, y in (("WIS1", img), ("WIS2", 1 - img)):
        piece = WI.at[1, pl.ds(aligned((1 - core) * dvh + y * dvq, dvq), dvq)]
        remote(piece, piece, sib, name).wait_recv()
    for bits in range(8):
        block = feat_block(bits, 1 - core)
        remote(block, block, sib, f"S{bits}").wait_recv()
    for copy in (locals_[1], locals_[3]):
        copy.wait()

    @pl.loop(0, stride)
    def _(t):
        block = inside + t % 2 - 2 * (t % 2) * (inside % 2)
        block = block + 2 * (t // 2) - 4 * (t // 2) * ((block // 2) % 2)
        first = block * rows + core * tile
        place = first + lax.broadcasted_iota(jnp.int32, (tile, 1), 0)
        row = lookup(place)
        kept = jnp.where(row >= 0, 1.0, 0.0).astype(F32)
        wanted = lax.broadcasted_iota(jnp.int32, (tile, tokens), 1) == row
        chosen = jnp.where(wanted, 1.0, 0.0).astype(BF16)
        values = jnp.dot(chosen, F[...], preferred_element_type=F32)
        here = pl.ds(aligned(t * tile, tile), tile)
        V[here] = values.astype(BF16)
        mean = jnp.mean(values, axis=1, keepdims=True)
        centred = values - mean
        rstd = lax.rsqrt(jnp.mean(centred * centred, axis=1, keepdims=True) + 1e-05)
        MEAN[here] = mean
        RSTD[here] = rstd
        scaled = centred * rstd * gain_ref[...] + bias_ref[...]
        normed_in = scaled.astype(BF16)
        NT[:, here] = scaled.T.astype(BF16)
        for g in range(samples):
            shift_row = bin_ref[...] if g == 0 else PB[...]
            preact = jnp.dot(normed_in, WI[g], preferred_element_type=F32) + shift_row
            activ, slope = gelu_parts(preact)
            columns = pl.ds(g * hb, hb)
            SL[here, columns] = slope * kept
            HT[columns, pl.ds(aligned(t * rows + core * tile, tile), tile)] = (
                (activ * kept).T.astype(BF16)
            )
        ht_copy(t).start()

        @pl.when(t == 2)
        def _():
            @pl.when(outer)
            def _():
                hand_wo(1)

    @pl.when(outer)
    def _():
        for k in range(1, EARLY_D):
            z_copy(k).wait_recv()
            d_copy(k).start()

    def y_copy(k):
        columns = pl.ds(aligned(k * ck, ck), ck)
        return remote(YS.at[:, columns], YR.at[:, columns], yn, "YK", k=k, count=PIECES)

    def zk_copy(k):
        columns = pl.ds(aligned(k * ck, ck), ck)
        return remote(ZS.at[:, columns], ZR.at[:, columns], z2, "ZK", k=k, count=PIECES)

    def weight_grad(k):
        columns = pl.ds(aligned(k * ck, ck), ck)
        piece = L[:, columns]
        for g in range(samples):
            mine = pl.ds(aligned(g * hb + img * hh, hh), hh)
            other = pl.ds(aligned(g * hb + (1 - img) * hh, hh), hh)
            sent = jnp.dot(HT[other], piece, preferred_element_type=F32)
            YS[pl.ds(g * hh, hh), columns] = sent.astype(BF16)
            kept = jnp.dot(HT[mine], piece, preferred_element_type=F32)
            if g == 0:
                wo_out[:, columns] = kept
            else:
                GP[:, columns] = kept
        y_copy(k).start()

    def hidden_part(k, s, g, low, size):
        columns = pl.ds(aligned(k * ck, ck), ck)
        HP[s, :, pl.ds(aligned(g * hb + low, hh), size)] += lax.dot_general(
            L[pl.ds(aligned(s * rows, rows), rows), columns],
            W[g, pl.ds(aligned(low, hh), size), columns],
            (((1,), (1,)), ((), ())),
            preferred_element_type=F32,
        )

    def half_rows(c):
        return pl.ds(aligned(c * tile, tile), tile)

    def exchange(s):
        PG[pl.ds(aligned(s * tile, tile), tile)] = HP[s, half_rows(1 - core)].astype(BF16)
        hr_copy(s).start()

    def preact_grad(s):
        copy = hr_copy(s)
        copy.wait()
        here = pl.ds(s * tile, tile)
        grad = HP[s, half_rows(core)] + HR[here].astype(F32)
        rounded = (grad * SL[here]).astype(BF16)
        PG[here] = rounded
        ACC[pl.ds(0, 1)] += jnp.sum(rounded.astype(F32), axis=0, keepdims=True)

    def over_img(k):
        columns = pl.ds(aligned(k * ck, ck), ck)
        y_copy(k).wait_recv()
        wo_out[:, columns] += YR[pl.ds(0, hh), columns].astype(F32)
        both = GP[:, columns] + YR[pl.ds(hh, hh), columns].astype(F32)
        ZS[:, columns] = both.astype(BF16)
        zk_copy(k).start()

    def over_samples(k):
        columns = pl.ds(aligned(k * ck, ck), ck)
        zk_copy(k).wait_recv()
        wo_out[:, columns] += ZR[:, columns].astype(F32)

    ACC[...] = jnp.zeros(ACC.shape, F32)

    last = stride - 1

    def hidden_parts(k, s):
        hidden_part(k, s, 0, 0, hb)
        for n in range(LATE_MINE, PIECES):

            @pl.when(k == n)
            def _():
                for late, step, y in ((LATE_MINE, 2, img), (LATE, 2, 1 - img)):
                    low = min(step * (n - late), n)
                    high = min(step * (n - late) + step, n + 1)
                    if n >= late:

                        @pl.loop(low, high)
                        def _(j):
                            for g in range(1, samples):
                                hidden_part(j, s, g, y * hh, hh)

    @pl.loop(0, PIECES)
    def _(k):
        x_copy(k).wait_recv()

        @pl.when(k == LATE)
        def _():
            for n in range(2):
                piece = W.at[1, wo_piece(1 - img, n)]
                remote(piece, piece, yn, f"WY{n}").wait_recv()

        @pl.loop(0, last)
        def _(s):
            hidden_parts(k, s)

            @pl.when(k == PIECES - 1)
            def _():
                exchange(s)

        d_copy(k).wait_recv()
        @pl.when(k == 0)
        def _():
            for t in range(stride):
                piece = ht_piece(t, 1 - core)
                remote(piece, piece, sib, "HT", k=t, count=stride).wait_recv()

        weight_grad(k)

        @pl.when(k >= 1)
        def _():
            over_img(k - 1)

        hidden_parts(k, last)

        @pl.when(k == PIECES - 1)
        def _():
            exchange(last)

        @pl.when(k + EARLY_D < PIECES)
        def _():
            z_copy(k + EARLY_D).wait_recv()
            d_copy(k + EARLY_D).start()

        @pl.when(k == 1)
        def _():
            @pl.when(inner)
            def _():
                hand_wo(1)

        for n in range(LATE_X, PIECES):

            @pl.when(k == n - LATE_X)
            def _():
                x_copy(n).start()


    for s in range(last):
        preact_grad(s)
    preact_grad(last)

    def first_grad(block):
        lines = pl.ds(aligned(block * dvq, dvq), dvq)
        return jnp.dot(NT[lines], PG[...], preferred_element_type=F32)

    mine_rows = pl.ds(aligned(img * dvq, dvq), dvq)
    other_rows = pl.ds(aligned((1 - img) * dvq, dvq), dvq)
    own_cols = pl.ds(0, hb)
    far_cols = [pl.ds(hb + n * (hb // 2), hb // 2) for n in range(2)]

    def send_img():
        WYS[...] = HP[0, other_rows].astype(BF16)
        for n in range(2):
            start(WYS.at[:, far_cols[n]], WYR.at[:, far_cols[n]], yn, f"WYF{n}")
        start(WYS.at[:, own_cols], WYR.at[:, own_cols], yn, "WYO")

    def kept_rows(y):
        return pl.ds(aligned(y * dvq, dvq), dvq)

    def wg_copy(n, y):
        return remote(WS.at[y], WR.at[y], sib, f"WG{n}")

    for n, y in enumerate((1 - img, img)):
        WS[y] = first_grad(2 * y + 1 - core).astype(BF16)
        wg_copy(n, y).start()
        HP[0, kept_rows(y)] = first_grad(2 * y + core)
        if n == 0:
            wg_copy(n, y).wait_recv()
            HP[0, kept_rows(y)] += WR[y].astype(F32)
            send_img()
            over_img(PIECES - 1)
    wg_copy(1, img).wait_recv()
    def over_far(n):
        local = pl.ds(n * (hb // 2), hb // 2)
        columns = far_cols[n]
        remote(WYS.at[:, columns], WYR.at[:, columns], yn, f"WYF{n}").wait_recv()
        total = HP[0, mine_rows, columns] + WR[img, :, columns].astype(F32)
        WZS[:, local] = (total + WYR[:, columns].astype(F32)).astype(BF16)
        start(WZS.at[:, local], WZR.at[:, local], z2, f"WZS{n}")


    @pl.loop(0, part // tile)
    def _(t):
        here = pl.ds(aligned(t * tile, tile), tile)
        grad = jnp.zeros((tile, dv), F32)
        for g in range(samples):
            grad = grad + lax.dot_general(
                PG[here, pl.ds(g * hb, hb)],
                WI[g],
                (((1,), (1,)), ((), ())),
                preferred_element_type=F32,
            )
        normed = (V[here].astype(F32) - MEAN[here]) * RSTD[here]
        ACC[pl.ds(1, 1)] += jnp.sum(grad * normed, axis=0, keepdims=True)
        ACC[pl.ds(2, 1)] += jnp.sum(grad, axis=0, keepdims=True)

    put_small(gain_row, ACC[pl.ds(1, 1)][:, :dv])
    put_small(bias_row, ACC[pl.ds(2, 1)][:, :dv])
    sums = ACC[pl.ds(0, 1)]
    for g in range(samples):
        put_small(
            b_in_row + flip(seq, 4 * g) * (hb // lanes), sums[:, g * hb : (g + 1) * hb]
        )

    def small_start(n, target, place=None):
        place = n if place is None else place
        start(SV.at[n], AR.at[place], target, f"AR{place}")

    def small_wait(n):
        remote(SV.at[0], AR.at[n], sib, f"AR{n}").wait_recv()

    small_start(0, sib)
    over_far(0)
    over_far(1)
    small_wait(0)
    SV[1] = SV[0] + AR[0]
    small_start(1, xn)
    small_wait(1)
    SV[2] = SV[1] + AR[1]
    small_start(2, yn)
    small_wait(2)
    SV[3] = SV[2] + AR[2]
    for n, target in enumerate((z1, z2, z3)):
        small_start(3, target, 3 + n)
    remote(WYS.at[:, own_cols], WYR.at[:, own_cols], yn, "WYO").wait_recv()
    wi_out[...] = (HP[0, mine_rows, own_cols] + WR[img, :, own_cols].astype(F32)
                   + WYR[:, own_cols].astype(F32))
    def wo_store(k):
        columns = pl.ds(aligned(k * ck, ck), ck)
        return pltpu.make_async_copy(
            wo_out.at[:, columns], wo_hbm.at[:, columns], out_sem.at[k]
        )

    @pl.loop(0, PIECES)
    def _(k):
        over_samples(k)
        wo_store(k).start()

    for n in range(2):
        local = pl.ds(n * (hb // 2), hb // 2)
        remote(WZS.at[:, local], WZR.at[:, local], z2, f"WZS{n}").wait_recv()
        wi_out[:, local] += WZR[:, local].astype(F32)
    for n in range(3, 6):
        small_wait(n)
    small_out[...] = (SV[3] + AR[3]) + (AR[4] + AR[5])
    stores = [pltpu.make_async_copy(wi_out, wi_hbm, out_sem.at[PIECES])]
    row = 0
    for n, ref in enumerate((gain_hbm, bias_hbm, b_in_hbm, b_out_hbm)):
        piece = small_out.at[pl.ds(row, ref.shape[0])]
        stores.append(pltpu.make_async_copy(piece, ref, out_sem.at[PIECES + 1 + n]))
        row += ref.shape[0]
    for copy in stores:
        copy.start()
    for copy in started:
        copy.wait_send()

    @pl.when(inner)
    def _():
        for copy in (cut_own, cut_pair, back_near, back_far):
            copy.wait_send()

    for n in range(2):
        piece = W.at[1, wo_piece(img, n)]
        remote(piece, piece, yn, f"WY{n}").wait_send()
    for t in range(stride):
        ht_copy(t).wait_send()
    for copy in (wi_copy, *wo_copies, wg_copy(0, 1 - img), wg_copy(1, img)):
        copy.wait_send()

    @pl.loop(0, PIECES)
    def _(k):
        for copy in (x_copy, z_copy, d_copy, y_copy, zk_copy):
            copy(k).wait_send()

    @pl.loop(0, PIECES)
    def _(k):
        wo_store(k).wait()

    for copy in stores:
        copy.wait()


def finish_body(ins, outs, held, sems):
    pieces = []
    for source, place, target in zip(ins, held, outs):
        lines = source.shape[0]
        step = lines // 4 if lines >= 128 else lines
        for low in range(0, lines, step):
            rows = pl.ds(low, step)
            pieces.append((source.at[rows], place.at[rows], target.at[rows]))
    copies = []
    for n, (source, place, _) in enumerate(pieces):
        copies.append(pltpu.make_async_copy(source, place, sems.at[0, n]))
        copies[-1].start()
    later = []
    for n, (_, place, target) in enumerate(pieces):
        copies[n].wait()
        later.append(pltpu.make_async_copy(place, target, sems.at[1, n]))
        later[-1].start()
    for copy in later:
        copy.wait()


def finish(values):
    count = len(values)
    hbm = pl.BlockSpec(memory_space=pl.ANY)

    def body(*refs):
        finish_body(refs[:count], refs[count : 2 * count], refs[2 * count : -1], refs[-1])

    return pl.pallas_call(
        body,
        out_shape=[jax.ShapeDtypeStruct(v.shape, v.dtype) for v in values],
        in_specs=[hbm] * count,
        out_specs=[hbm] * count,
        scratch_shapes=[pltpu.VMEM(v.shape, v.dtype) for v in values]
        + [pltpu.SemaphoreType.DMA((2, 4 * count))],
    )(*values)


def per_device_kernel(
    vision_feats, ln_gain, ln_bias, w_in, b_in, w_out, lm_grad, image_counts, token_pos
):
    seq_count = lax.axis_size("seq")
    _, rows, half = lm_grad.shape
    hb = w_out.shape[0]
    dv = ln_gain.shape[0]
    frows = vision_feats.shape[1]
    tokens = token_pos.shape[1]
    samples = image_counts.shape[1]
    stride = seq_count // samples
    span = stride * rows
    part = span // 2
    hid = samples * hb
    images = tokens // PATCH
    lanes = 128
    small = (2 * dv + seq_count * hb + 2 * half) // lanes
    dims = (rows, half, hb, dv, frows, tokens, seq_count, samples, images)
    vmem = pl.BlockSpec(memory_space=pltpu.VMEM)
    smem = pl.BlockSpec(memory_space=pltpu.SMEM)
    hbm = pl.BlockSpec(memory_space=pl.ANY)
    wo, wi, *sums = pl.pallas_call(
        functools.partial(kernel_body, dims),
        out_shape=(
            jax.ShapeDtypeStruct((hb // 2, half), F32),
            jax.ShapeDtypeStruct((dv // 4, hb), F32),
            jax.ShapeDtypeStruct((dv // lanes, lanes), F32),
            jax.ShapeDtypeStruct((dv // lanes, lanes), F32),
            jax.ShapeDtypeStruct((seq_count * hb // lanes, lanes), F32),
            jax.ShapeDtypeStruct((2 * half // lanes, lanes), F32),
        ),
        in_specs=[smem, smem, hbm, vmem, vmem, hbm, vmem, hbm, hbm],
        out_specs=[hbm] * 6,
        scratch_shapes=[
            pltpu.VMEM((span, half), BF16),
            pltpu.VMEM((samples, hb, half), BF16),
            pltpu.VMEM((samples, dv, hb), BF16),
            pltpu.VMEM((tokens, dv), BF16),
            pltpu.VMEM((dv, part), BF16),
            pltpu.VMEM((part, dv), BF16),
            pltpu.VMEM((part, 1), F32),
            pltpu.VMEM((part, 1), F32),
            pltpu.VMEM((part, hid), F32),
            pltpu.VMEM((hid, span), BF16),
            pltpu.VMEM((stride, rows, hid), F32),
            pltpu.VMEM((part, hid), BF16),
            pltpu.VMEM((part, hid), BF16),
            pltpu.VMEM((hb, half), BF16),
            pltpu.VMEM((hb, half), BF16),
            pltpu.VMEM((hb // 2, half), BF16),
            pltpu.VMEM((hb // 2, half), BF16),
            pltpu.VMEM((hb // 2, half), F32),
            pltpu.VMEM((2, dv // 4, hid), BF16),
            pltpu.VMEM((2, dv // 4, hid), BF16),
            pltpu.VMEM((dv // 4, hid), BF16),
            pltpu.VMEM((dv // 4, hid), BF16),
            pltpu.VMEM((dv // 4, hb), BF16),
            pltpu.VMEM((dv // 4, hb), BF16),
            pltpu.VMEM((1, hb), F32),
            pltpu.VMEM((8, max(hid, dv)), F32),
            pltpu.VMEM((4, small, lanes), F32),
            pltpu.VMEM((6, small, lanes), F32),
            pltpu.VMEM((hb // 2, half), F32),
            pltpu.VMEM((dv // 4, hb), F32),
            pltpu.VMEM((small, lanes), F32),
            pltpu.SemaphoreType.DMA((PIECES + 5,)),
            pltpu.SemaphoreType.DMA((96,)),
            pltpu.SemaphoreType.DMA((96,)),
            pltpu.SemaphoreType.DMA((4,)),
        ],
        compiler_params=pltpu.CompilerParams(
            collective_id=0, has_side_effects=True, vmem_limit_bytes=67043328
        ),
    )(
        image_counts,
        token_pos,
        vision_feats[0],
        ln_gain[None],
        ln_bias[None],
        w_in,
        b_in[None],
        w_out,
        lm_grad[0],
    )
    wo, wi, *sums = finish((wo, wi, *sums))
    gain_grad, bias_grad, b_in_grad, b_out_grad = (value.reshape(-1) for value in sums)
    return (wi, b_in_grad, wo, b_out_grad, gain_grad, bias_grad)


def dispatch(mesh, *args):
    sizes = (mesh.shape["seq"], mesh.shape["img"], mesh.shape["fsdp"])
    if sizes == (8, 2, 2) and args[7].shape[1] == 2:
        return per_device_kernel(*args)
    return per_device(*args)


def solution(mesh):
    return jax.shard_map(
        functools.partial(dispatch, mesh),
        mesh=mesh,
        in_specs=(
            P("img", ("seq", "fsdp"), None),
            P(),
            P(),
            P("fsdp", "seq"),
            P("seq"),
            P("seq", "fsdp"),
            P("img", "seq", "fsdp"),
            P("img", None),
            P("img", None),
        ),
        out_specs=(
            P(("img", "fsdp"), "seq"),
            P(),
            P(("seq", "img"), "fsdp"),
            P(),
            P(),
            P(),
        ),
        check_vma=False,
    )
```

```python
import functools

import jax
import jax.numpy as jnp
from jax import lax
from jax.experimental import pallas as pl
from jax.experimental.pallas import tpu as pltpu
from jax.sharding import PartitionSpec as P

PATCH = 576
CHUNKS = 2
PIECES = 8
EARLY_X = 4
EARLY_D = 2
LATE_X = 6
LATE_MINE = 2
LATE = 3
BF16 = jnp.bfloat16
F32 = jnp.float32


def gelu_parts(preact):
    cumul = 0.5 * (1.0 + lax.erf(preact * 0.7071067811865476))
    density = jnp.exp(-0.5 * preact * preact) * 0.3989422804014327
    return (preact * cumul, cumul + preact * density)


def contract(left, right, left_dim, right_dim):
    return lax.dot_general(
        left, right, (((left_dim,), (right_dim,)), ((), ())), preferred_element_type=jnp.float32
    )


def shift(value, axis, amount):
    count = lax.axis_size(axis)
    return lax.ppermute(value, axis, [(i, (i + amount) % count) for i in range(count)])


def flip(value, bit):
    count = lax.axis_size("seq")
    return lax.ppermute(value, "seq", [(i, i ^ bit) for i in range(count)])


def pick(value, index, axis):
    return lax.dynamic_index_in_dim(value, index, axis=axis, keepdims=False)


def scatter_sum(value, axis):
    count = lax.axis_size(axis)
    index = lax.axis_index(axis)
    if count > 2:
        return lax.psum_scatter(value, axis, scatter_dimension=0, tiled=False)
    if count == 1:
        return value[0]
    sent = pick(value, 1 - index, 0).astype(jnp.bfloat16)
    return pick(value, index, 0) + shift(sent, axis, 1).astype(jnp.float32)


def sample_sum(value, stride, after):
    total, _ = lax.optimization_barrier((value[0], after))
    for k in range(1, value.shape[0]):
        moved = shift(value[k].astype(jnp.bfloat16), "seq", -k * stride)
        total = total + moved.astype(jnp.float32)
    return total


def per_device(vision_feats, ln_gain, ln_bias, w_in, b_in, w_out, lm_grad, image_counts, token_pos):
    seq_count = lax.axis_size("seq")
    seq_index = lax.axis_index("seq")
    img_count = lax.axis_size("img")
    fsdp_count = lax.axis_size("fsdp")
    fsdp_index = lax.axis_index("fsdp")
    lm_block = lm_grad[0]
    block_rows, half_width = lm_block.shape
    counts = image_counts[0]
    samples = counts.shape[0]
    stride = seq_count // samples
    sample_len = stride * block_rows
    own_sample = seq_index // stride
    positions = token_pos[0]
    row_count = positions.shape[0]
    images = row_count // PATCH
    starts = positions.reshape(images, PATCH)[:, 0]
    bounds = jnp.cumsum(counts)
    image_index = jnp.arange(images, dtype=jnp.int32)
    image_sample = jnp.sum((image_index[:, None] >= bounds[None, :]).astype(jnp.int32), axis=1)
    in_sample = image_sample == own_sample

    def lookup(place):
        offset = place[:, None] - starts[None, :]
        match = in_sample[None, :] & (offset >= 0) & (offset < PATCH)
        row = jnp.sum(jnp.where(match, offset + image_index[None, :] * PATCH, 0), axis=1)
        return row, jnp.any(match, axis=1)

    own_place = (seq_index % stride) * block_rows + jnp.arange(block_rows, dtype=jnp.int32)
    own_mask = lookup(own_place)[1].astype(jnp.bfloat16)
    out_bias_half = jnp.dot(own_mask[None, :], lm_block, preferred_element_type=jnp.float32)[0]
    out_bias_whole = lax.dynamic_update_slice_in_dim(
        jnp.zeros((half_width * fsdp_count,), jnp.float32),
        out_bias_half,
        fsdp_index * half_width,
        0,
    )

    feats = lax.all_gather(vision_feats[0], ("seq", "fsdp"), axis=0, tiled=True)

    in_blocks = [w_in] + [shift(w_in, "seq", k * stride) for k in range(1, samples)]
    in_bias = jnp.concatenate([b_in] + [shift(b_in, "seq", k * stride) for k in range(1, samples)])
    w_in_half = jnp.concatenate(in_blocks, axis=1)
    w_in_full = lax.all_gather(w_in_half, "fsdp", axis=0, tiled=True)
    w_out_later, _ = lax.optimization_barrier((w_out, w_in_half))
    w_out_full = jnp.concatenate(
        [w_out] + [shift(w_out_later, "seq", k * stride) for k in range(1, samples)], axis=0
    )
    hid = in_bias.shape[0]
    block_hid = hid // samples

    groups = [[s * stride + i for i in range(stride)] for s in range(samples)]
    width = half_width // CHUNKS
    slices = [lm_block[:, c * width : (c + 1) * width] for c in range(CHUNKS)]
    crossed = stride == 4
    if crossed:
        pieces = []
        for piece in slices:
            far = flip(piece, 2)
            near = flip(piece, 1)
            pieces.append(jnp.concatenate([piece, near, far, flip(far, 1)], axis=0))
    else:
        pieces = [
            lax.all_gather(piece, "seq", axis=0, tiled=True, axis_index_groups=groups)
            for piece in slices
        ]
    b_out_grad = lax.psum(out_bias_whole, ("seq", "img", "fsdp"))
    feats, b_out_grad = lax.optimization_barrier((feats, b_out_grad))

    part_len = sample_len // fsdp_count
    place = fsdp_index * part_len + jnp.arange(part_len, dtype=jnp.int32)
    if crossed:
        block = place // block_rows
        place = (block ^ (seq_index % stride)) * block_rows + place % block_rows
    row, mask = lookup(place)
    values = feats.at[row].get(mode="promise_in_bounds").astype(jnp.float32)
    row_mean = jnp.mean(values, axis=1, keepdims=True)
    centred = values - row_mean
    row_var = jnp.mean(centred * centred, axis=1, keepdims=True)
    normed = centred * lax.rsqrt(row_var + 1e-05)
    normed_in = (normed * ln_gain + ln_bias).astype(jnp.bfloat16)
    preact = jnp.dot(normed_in, w_in_full, preferred_element_type=jnp.float32) + in_bias
    activ, slope = gelu_parts(preact)
    hidden = jnp.where(mask[:, None], activ, 0.0).astype(jnp.bfloat16)
    slope = jnp.where(mask[:, None], slope, 0.0)
    if fsdp_count == 2:
        other = shift(hidden, "fsdp", 1)
        first = fsdp_index == 0
        hidden_full = jnp.concatenate(
            [jnp.where(first, hidden, other), jnp.where(first, other, hidden)], axis=0
        )
    else:
        hidden_full = lax.all_gather(hidden, "fsdp", axis=0, tiled=True)

    w_out_grads = []
    hidden_part = 0.0
    hidden_full, pieces[0] = lax.optimization_barrier((hidden_full, pieces[0]))
    for c in range(CHUNKS):
        piece = pieces[c]
        part = contract(hidden_full, piece, 0, 0)
        part = part.reshape(samples, img_count, block_hid // img_count, width)
        part = scatter_sum(part.transpose(1, 0, 2, 3), "img")
        w_out_grads.append(part)
        hidden_part = hidden_part + contract(
            piece, w_out_full[:, c * width : (c + 1) * width], 1, 1
        )

    hidden_grad = scatter_sum(hidden_part.reshape(fsdp_count, part_len, hid), "fsdp")
    preact_grad = (hidden_grad * slope).astype(jnp.bfloat16)
    in_part = contract(normed_in, preact_grad, 0, 0)
    in_part = in_part.reshape(img_count, fsdp_count, -1, samples, block_hid)
    in_part = scatter_sum(in_part.transpose(1, 0, 2, 3, 4), "fsdp")
    in_part = scatter_sum(in_part, "img")

    b_in_part = jnp.sum(preact_grad, axis=0, dtype=jnp.float32)
    normed_grad = contract(preact_grad, w_in_full, 1, 1)
    gain_part = jnp.sum(normed_grad * normed, axis=0)
    bias_part = jnp.sum(normed_grad, axis=0)
    hidden_bias = jnp.zeros((seq_count, block_hid), jnp.float32)
    for k in range(samples):
        owner = (seq_index - k * stride + seq_count) % seq_count
        hidden_bias = lax.dynamic_update_slice(
            hidden_bias, b_in_part[None, k * block_hid : (k + 1) * block_hid], (owner, 0)
        )
    gain_grad, bias_grad, b_in_grad = lax.psum(
        (gain_part, bias_part, hidden_bias.reshape(-1)), ("seq", "img", "fsdp")
    )
    w_in_grad = sample_sum(in_part.transpose(1, 0, 2), stride, gain_grad)
    w_out_grad = jnp.concatenate(
        [sample_sum(part, stride, gain_grad) for part in w_out_grads], axis=1
    )
    return (w_in_grad, b_in_grad, w_out_grad, b_out_grad, gain_grad, bias_grad)


def kernel_body(
    dims,
    counts_ref,
    pos_ref,
    feats_ref,
    gain_ref,
    bias_ref,
    wi_ref,
    bin_ref,
    wo_ref,
    lm_ref,
    wo_hbm,
    wi_hbm,
    gain_hbm,
    bias_hbm,
    b_in_hbm,
    b_out_hbm,
    L,
    W,
    WI,
    F,
    NT,
    V,
    MEAN,
    RSTD,
    SL,
    HT,
    HP,
    PG,
    HR,
    YS,
    YR,
    ZS,
    ZR,
    GP,
    WS,
    WR,
    WYS,
    WYR,
    WZS,
    WZR,
    PB,
    ACC,
    SV,
    AR,
    wo_out,
    wi_out,
    small_out,
    out_sem,
    send_sem,
    recv_sem,
    local_sem,
):
    rows, half, hb, dv, frows, tokens, seq_count, samples, images = dims
    stride = seq_count // samples
    span = stride * rows
    part = span // 2
    hid = samples * hb
    hh = hb // 2
    dvh = dv // 2
    dvq = dv // 4
    ck = half // PIECES
    seq = lax.axis_index("seq")
    img = lax.axis_index("img")
    core = lax.axis_index("fsdp")

    def flip(value, bits):
        for bit in (1, 2, 4):
            if bits & bit:
                value = value + bit - 2 * bit * ((value // bit) % 2)
        return value

    def device(bits=0, y=0, c=0):
        return (
            flip(seq, bits),
            1 - img if y else img,
            1 - core if c else core,
        )

    z1 = device(2)
    z2 = device(4)
    z3 = device(6)
    xn = device(1)
    yn = device(y=1)
    sib = device(c=1)

    names = {}

    def slot(name, count=1):
        if name not in names:
            names[name] = sum(c for _, c in names.values()), count
        return names[name][0]

    def remote(src, dst, target, recv, send=None, k=0, count=1):
        return pltpu.make_async_remote_copy(
            src_ref=src,
            dst_ref=dst,
            send_sem=send_sem.at[slot(send or recv, count) + k],
            recv_sem=recv_sem.at[slot(recv, count) + k],
            device_id=target,
            device_id_type=pl.DeviceIdType.MESH,
        )

    started = []

    def start(*args, **kwargs):
        copy = remote(*args, **kwargs)
        copy.start()
        started.append(copy)

    def aligned(value, unit):
        return pl.multiple_of(value, unit)

    def feat_block(bits, c):
        return F.at[pl.ds(aligned((flip(seq, bits) * 2 + c) * frows, 16), frows)]

    inside = seq % stride
    sample = seq // stride
    bounds = [counts_ref[0, 0] * 0]
    for s in range(samples):
        bounds.append(bounds[-1] + counts_ref[0, s])
    low = bounds[0]
    high = bounds[1]
    for s in range(1, samples):
        low = jnp.where(sample == s, bounds[s], low)
        high = jnp.where(sample == s, bounds[s + 1], high)
    begins = []
    for n in range(images):
        here = jnp.where(n >= low, jnp.where(n < high, 1, 0), 0)
        begins.append(jnp.where(here == 1, pos_ref[0, n * PATCH], 2 * span))

    def lookup(place):
        row = jnp.full(place.shape, -1, jnp.int32)
        for n in range(images):
            offset = place - begins[n]
            match = jnp.logical_and(offset >= 0, offset < PATCH)
            row = jnp.where(match, offset + n * PATCH, row)
        return row

    lanes = SV.shape[2]
    gain_row, bias_row = 0, dv // lanes
    b_in_row = 2 * (dv // lanes)
    b_out_row = b_in_row + seq_count * (hb // lanes)

    def put_small(row, value):
        for m in range(value.shape[1] // lanes):
            SV[0, pl.ds(row + m, 1)] = value[:, m * lanes : (m + 1) * lanes]

    def own_sums():
        place = inside * rows + lax.broadcasted_iota(jnp.int32, (rows, 1), 0)
        own_kept = jnp.where(lookup(place) >= 0, 1.0, 0.0).astype(F32)
        for m in range(half // hb):
            block = L[pl.ds(0, rows), pl.ds(m * hb, hb)].astype(F32) * own_kept
            total = jnp.sum(block, axis=0, keepdims=True)
            put_small(b_out_row + core * (half // lanes) + m * (hb // lanes), total)

    barrier = pltpu.get_barrier_semaphore()
    for target in (z1, z2, z3, xn, yn, sib):
        pl.semaphore_signal(
            barrier, inc=1, device_id=target, device_id_type=pl.DeviceIdType.MESH
        )

    locals_ = [
        pltpu.make_async_copy(feats_ref, feat_block(0, core), local_sem.at[0]),
        pltpu.make_async_copy(
            wi_ref, WI.at[0, pl.ds(aligned(core * dvh, dvh), dvh)], local_sem.at[1]
        ),
        pltpu.make_async_copy(lm_ref, L.at[pl.ds(0, rows)], local_sem.at[2]),
        pltpu.make_async_copy(wo_ref, W.at[0], local_sem.at[3]),
    ]
    for copy in locals_:
        copy.start()
    pl.semaphore_wait(barrier, 6)

    def lm_piece(k, index):
        columns = pl.ds(aligned(k * ck, ck), ck)
        return L.at[pl.ds(index * rows, rows), columns]

    def lm_own(k):
        return lm_ref.at[:, pl.ds(aligned(k * ck, ck), ck)]

    def x_copy(k):
        return remote(lm_own(k), lm_piece(k, 1), xn, "X", k=k, count=PIECES)

    def z_copy(k):
        return remote(lm_own(k), lm_piece(k, 2), z1, "Z", k=k, count=PIECES)

    def d_copy(k):
        return remote(lm_piece(k, 2), lm_piece(k, 3), xn, "D", k=k, count=PIECES)

    zseq = seq // 2
    inner = (zseq + 1) // 2 == 1

    def ht_copy(t):
        return remote(ht_piece(t, core), ht_piece(t, core), sib, "HT", k=t, count=stride)

    def hr_copy(s):
        here = pl.ds(aligned(s * tile, tile), tile)
        return remote(PG.at[here], HR.at[here], sib, "HR", k=s, count=stride)
    wi_rows = pl.ds(aligned(img * dvq, dvq), dvq)
    wi_mine = WI.at[1, pl.ds(aligned(core * dvh + img * dvq, dvq), dvq)]
    wi_other = WI.at[1, pl.ds(aligned(core * dvh + (1 - img) * dvq, dvq), dvq)]
    quarter = hh // 2

    def wo_piece(y, n):
        return pl.ds(aligned(y * hh + n * quarter, quarter), quarter)

    def hand_wo(n):
        piece = W.at[1, wo_piece(img, n)]
        remote(piece, piece, z2, f"WZ{n}").wait_recv()
        remote(piece, piece, yn, f"WY{n}").start()

    def ht_piece(s, c):
        return HT.at[:, pl.ds(aligned(s * rows + c * tile, tile), tile)]

    tile = rows // 2

    start(feats_ref, feat_block(0, core), z1, "F2")
    start(bin_ref, PB, z2, "BZ")
    wi_copy = remote(wi_ref.at[wi_rows], wi_mine, z2, "WIZ")
    wo_copies = [
        remote(wo_ref.at[wo_piece(img, n)], W.at[1, wo_piece(img, n)], z2, f"WZ{n}")
        for n in range(2)
    ]
    outer = 1 - (zseq + 1) // 2 % 2 == 1

    @pl.when(inner)
    def _():
        wi_copy.start()

    z_copy(0).start()

    @pl.when(outer)
    def _():
        for k in range(1, 3):
            z_copy(k).start()
        wi_copy.start()
        wo_copies[0].start()
        for k in range(3, PIECES - 1):
            z_copy(k).start()
        wo_copies[1].start()
        z_copy(PIECES - 1).start()

    start(feats_ref, feat_block(0, core), xn, "F1")
    x_copy(0).start()
    start(feats_ref, feat_block(0, core), sib, "S0")
    start(wi_ref, WI.at[0, pl.ds(aligned(core * dvh, dvh), dvh)], sib, "WIS0")

    def arrive(bits, name):
        remote(feats_ref, feat_block(bits, core), xn, name).wait_recv()

    def hand_x(bits):
        block = feat_block(bits, core)
        start(block, block, xn, f"F{bits + 1}")

    def hand_sib(bits):
        block = feat_block(bits, core)
        start(block, block, sib, f"S{bits}")

    arrive(2, "F2")
    locals_[0].wait()
    own_block, pair_block = feat_block(0, core), feat_block(2, core)
    far_block, near_block = feat_block(4, core), feat_block(6, core)
    cut_own = remote(own_block, own_block, z3, "F6", send="C0")
    cut_pair = remote(pair_block, pair_block, z3, "F4", send="C1")
    back_near = remote(near_block, near_block, z1, "F4", send="C2")
    back_far = remote(far_block, far_block, z1, "F6", send="C3")

    @pl.when(inner)
    def _():
        cut_own.start()
        cut_pair.start()

    hand_x(2)
    hand_sib(2)
    x_copy(1).start()

    @pl.when(outer)
    def _():
        for k in range(2, EARLY_X):
            x_copy(k).start()

    HP[...] = jnp.zeros(HP.shape, F32)
    ACC[...] = jnp.zeros(ACC.shape, F32)
    SV[0] = jnp.zeros(SV.shape[1:], F32)
    locals_[2].wait()
    own_sums()
    arrive(4, "F4")
    arrive(6, "F6")

    @pl.when(inner)
    def _():
        back_near.start()
        back_far.start()
        for copy in wo_copies:
            copy.start()
        for k in range(1, PIECES):
            z_copy(k).start()

    for bits in (4, 6):
        hand_x(bits)
        hand_sib(bits)

    @pl.when(inner)
    def _():
        for k in range(2, EARLY_X):
            x_copy(k).start()

    z_copy(0).wait_recv()
    d_copy(0).start()
    wi_copy.wait_recv()
    start(wi_mine, wi_mine, yn, "WIY")
    start(wi_mine, wi_mine, sib, "WIS1")
    for bits in (1, 3, 5, 7):
        arrive(bits, f"F{bits}")
        hand_sib(bits)
    remote(wi_other, wi_other, yn, "WIY").wait_recv()
    start(wi_other, wi_other, sib, "WIS2")
    @pl.when(inner)
    def _():
        for k in range(1, EARLY_D):
            z_copy(k).wait_recv()
            d_copy(k).start()

    for k in range(EARLY_X, LATE_X):
        x_copy(k).start()
    hand_wo(0)
    remote(bin_ref, PB, z2, "BZ").wait_recv()
    remote(
        wi_ref, WI.at[0, pl.ds(aligned((1 - core) * dvh, dvh), dvh)], sib, "WIS0"
    ).wait_recv()
    for name, y in (("WIS1", img), ("WIS2", 1 - img)):
        piece = WI.at[1, pl.ds(aligned((1 - core) * dvh + y * dvq, dvq), dvq)]
        remote(piece, piece, sib, name).wait_recv()
    for bits in range(8):
        block = feat_block(bits, 1 - core)
        remote(block, block, sib, f"S{bits}").wait_recv()
    for copy in (locals_[1], locals_[3]):
        copy.wait()

    @pl.loop(0, stride)
    def _(t):
        block = inside + t % 2 - 2 * (t % 2) * (inside % 2)
        block = block + 2 * (t // 2) - 4 * (t // 2) * ((block // 2) % 2)
        first = block * rows + core * tile
        place = first + lax.broadcasted_iota(jnp.int32, (tile, 1), 0)
        row = lookup(place)
        kept = jnp.where(row >= 0, 1.0, 0.0).astype(F32)
        wanted = lax.broadcasted_iota(jnp.int32, (tile, tokens), 1) == row
        chosen = jnp.where(wanted, 1.0, 0.0).astype(BF16)
        values = jnp.dot(chosen, F[...], preferred_element_type=F32)
        here = pl.ds(aligned(t * tile, tile), tile)
        V[here] = values.astype(BF16)
        mean = jnp.mean(values, axis=1, keepdims=True)
        centred = values - mean
        rstd = lax.rsqrt(jnp.mean(centred * centred, axis=1, keepdims=True) + 1e-05)
        MEAN[here] = mean
        RSTD[here] = rstd
        scaled = centred * rstd * gain_ref[...] + bias_ref[...]
        normed_in = scaled.astype(BF16)
        NT[:, here] = scaled.T.astype(BF16)
        for g in range(samples):
            shift_row = bin_ref[...] if g == 0 else PB[...]
            preact = jnp.dot(normed_in, WI[g], preferred_element_type=F32) + shift_row
            activ, slope = gelu_parts(preact)
            columns = pl.ds(g * hb, hb)
            SL[here, columns] = slope * kept
            HT[columns, pl.ds(aligned(t * rows + core * tile, tile), tile)] = (
                (activ * kept).T.astype(BF16)
            )
        ht_copy(t).start()

        @pl.when(t == 2)
        def _():
            @pl.when(outer)
            def _():
                hand_wo(1)

    @pl.when(outer)
    def _():
        for k in range(1, EARLY_D):
            z_copy(k).wait_recv()
            d_copy(k).start()

    def y_copy(k):
        columns = pl.ds(aligned(k * ck, ck), ck)
        return remote(YS.at[:, columns], YR.at[:, columns], yn, "YK", k=k, count=PIECES)

    def zk_copy(k):
        columns = pl.ds(aligned(k * ck, ck), ck)
        return remote(ZS.at[:, columns], ZR.at[:, columns], z2, "ZK", k=k, count=PIECES)

    def weight_grad(k):
        columns = pl.ds(aligned(k * ck, ck), ck)
        piece = L[:, columns]
        for g in range(samples):
            mine = pl.ds(aligned(g * hb + img * hh, hh), hh)
            other = pl.ds(aligned(g * hb + (1 - img) * hh, hh), hh)
            sent = jnp.dot(HT[other], piece, preferred_element_type=F32)
            YS[pl.ds(g * hh, hh), columns] = sent.astype(BF16)
            kept = jnp.dot(HT[mine], piece, preferred_element_type=F32)
            if g == 0:
                wo_out[:, columns] = kept
            else:
                GP[:, columns] = kept
        y_copy(k).start()

    def hidden_part(k, s, g, low, size):
        columns = pl.ds(aligned(k * ck, ck), ck)
        HP[s, :, pl.ds(aligned(g * hb + low, hh), size)] += lax.dot_general(
            L[pl.ds(aligned(s * rows, rows), rows), columns],
            W[g, pl.ds(aligned(low, hh), size), columns],
            (((1,), (1,)), ((), ())),
            preferred_element_type=F32,
        )

    def half_rows(c):
        return pl.ds(aligned(c * tile, tile), tile)

    def exchange(s):
        PG[pl.ds(aligned(s * tile, tile), tile)] = HP[s, half_rows(1 - core)].astype(BF16)
        hr_copy(s).start()

    def preact_grad(s):
        copy = hr_copy(s)
        copy.wait()
        here = pl.ds(s * tile, tile)
        grad = HP[s, half_rows(core)] + HR[here].astype(F32)
        rounded = (grad * SL[here]).astype(BF16)
        PG[here] = rounded
        ACC[pl.ds(0, 1)] += jnp.sum(rounded.astype(F32), axis=0, keepdims=True)

    def over_img(k):
        columns = pl.ds(aligned(k * ck, ck), ck)
        y_copy(k).wait_recv()
        wo_out[:, columns] += YR[pl.ds(0, hh), columns].astype(F32)
        both = GP[:, columns] + YR[pl.ds(hh, hh), columns].astype(F32)
        ZS[:, columns] = both.astype(BF16)
        zk_copy(k).start()

    def over_samples(k):
        columns = pl.ds(aligned(k * ck, ck), ck)
        zk_copy(k).wait_recv()
        wo_out[:, columns] += ZR[:, columns].astype(F32)

    ACC[...] = jnp.zeros(ACC.shape, F32)

    last = stride - 1

    def hidden_parts(k, s):
        hidden_part(k, s, 0, 0, hb)
        for n in range(LATE_MINE, PIECES):

            @pl.when(k == n)
            def _():
                for late, step, y in ((LATE_MINE, 2, img), (LATE, 2, 1 - img)):
                    low = min(step * (n - late), n)
                    high = min(step * (n - late) + step, n + 1)
                    if n >= late:

                        @pl.loop(low, high)
                        def _(j):
                            for g in range(1, samples):
                                hidden_part(j, s, g, y * hh, hh)

    @pl.loop(0, PIECES)
    def _(k):
        x_copy(k).wait_recv()

        @pl.when(k == LATE)
        def _():
            for n in range(2):
                piece = W.at[1, wo_piece(1 - img, n)]
                remote(piece, piece, yn, f"WY{n}").wait_recv()

        @pl.loop(0, last)
        def _(s):
            hidden_parts(k, s)

            @pl.when(k == PIECES - 1)
            def _():
                exchange(s)

        d_copy(k).wait_recv()
        @pl.when(k == 0)
        def _():
            for t in range(stride):
                piece = ht_piece(t, 1 - core)
                remote(piece, piece, sib, "HT", k=t, count=stride).wait_recv()

        weight_grad(k)

        @pl.when(k >= 1)
        def _():
            over_img(k - 1)

        hidden_parts(k, last)

        @pl.when(k == PIECES - 1)
        def _():
            exchange(last)

        @pl.when(k + EARLY_D < PIECES)
        def _():
            z_copy(k + EARLY_D).wait_recv()
            d_copy(k + EARLY_D).start()

        @pl.when(k == 1)
        def _():
            @pl.when(inner)
            def _():
                hand_wo(1)

        for n in range(LATE_X, PIECES):

            @pl.when(k == n - LATE_X)
            def _():
                x_copy(n).start()


    for s in range(last):
        preact_grad(s)
    preact_grad(last)

    def first_grad(block):
        lines = pl.ds(aligned(block * dvq, dvq), dvq)
        return jnp.dot(NT[lines], PG[...], preferred_element_type=F32)

    mine_rows = pl.ds(aligned(img * dvq, dvq), dvq)
    other_rows = pl.ds(aligned((1 - img) * dvq, dvq), dvq)
    own_cols = pl.ds(0, hb)
    far_cols = [pl.ds(hb + n * (hb // 2), hb // 2) for n in range(2)]

    def send_img():
        WYS[...] = HP[0, other_rows].astype(BF16)
        for n in range(2):
            start(WYS.at[:, far_cols[n]], WYR.at[:, far_cols[n]], yn, f"WYF{n}")

    def kept_rows(y):
        return pl.ds(aligned(y * dvq, dvq), dvq)

    def wg_copy(n, y):
        return remote(WS.at[y], WR.at[y], sib, f"WG{n}")

    for n, y in enumerate((1 - img, img)):
        WS[y] = first_grad(2 * y + 1 - core).astype(BF16)
        wg_copy(n, y).start()
        HP[0, kept_rows(y)] = first_grad(2 * y + core)
        if n == 0:
            wg_copy(n, y).wait_recv()
            HP[0, kept_rows(y)] += WR[y].astype(F32)
            send_img()
            over_img(PIECES - 1)
    wg_copy(1, img).wait_recv()
    def over_far(n):
        local = pl.ds(n * (hb // 2), hb // 2)
        columns = far_cols[n]
        remote(WYS.at[:, columns], WYR.at[:, columns], yn, f"WYF{n}").wait_recv()
        total = HP[0, mine_rows, columns] + WR[img, :, columns].astype(F32)
        WZS[:, local] = (total + WYR[:, columns].astype(F32)).astype(BF16)
        start(WZS.at[:, local], WZR.at[:, local], z2, f"WZS{n}")


    @pl.loop(0, part // tile)
    def _(t):
        here = pl.ds(aligned(t * tile, tile), tile)
        grad = jnp.zeros((tile, dv), F32)
        for g in range(samples):
            grad = grad + lax.dot_general(
                PG[here, pl.ds(g * hb, hb)],
                WI[g],
                (((1,), (1,)), ((), ())),
                preferred_element_type=F32,
            )
        normed = (V[here].astype(F32) - MEAN[here]) * RSTD[here]
        ACC[pl.ds(1, 1)] += jnp.sum(grad * normed, axis=0, keepdims=True)
        ACC[pl.ds(2, 1)] += jnp.sum(grad, axis=0, keepdims=True)

    put_small(gain_row, ACC[pl.ds(1, 1)][:, :dv])
    put_small(bias_row, ACC[pl.ds(2, 1)][:, :dv])
    sums = ACC[pl.ds(0, 1)]
    for g in range(samples):
        put_small(
            b_in_row + flip(seq, 4 * g) * (hb // lanes), sums[:, g * hb : (g + 1) * hb]
        )

    def small_start(n, target, place=None):
        place = n if place is None else place
        start(SV.at[n], AR.at[place], target, f"AR{place}")

    def small_wait(n):
        remote(SV.at[0], AR.at[n], sib, f"AR{n}").wait_recv()

    small_start(0, sib)
    over_far(0)
    over_far(1)
    small_wait(0)
    SV[1] = SV[0] + AR[0]
    small_start(1, xn)
    small_wait(1)
    SV[2] = SV[1] + AR[1]
    small_start(2, yn)
    start(WYS.at[:, own_cols], WYR.at[:, own_cols], yn, "WYO")
    small_wait(2)
    SV[3] = SV[2] + AR[2]
    for n, target in enumerate((z1, z2, z3)):
        small_start(3, target, 3 + n)
    remote(WYS.at[:, own_cols], WYR.at[:, own_cols], yn, "WYO").wait_recv()
    wi_out[...] = (HP[0, mine_rows, own_cols] + WR[img, :, own_cols].astype(F32)
                   + WYR[:, own_cols].astype(F32))
    def wo_store(k):
        columns = pl.ds(aligned(k * ck, ck), ck)
        return pltpu.make_async_copy(
            wo_out.at[:, columns], wo_hbm.at[:, columns], out_sem.at[k]
        )

    @pl.loop(0, PIECES)
    def _(k):
        over_samples(k)
        wo_store(k).start()

    for n in range(2):
        local = pl.ds(n * (hb // 2), hb // 2)
        remote(WZS.at[:, local], WZR.at[:, local], z2, f"WZS{n}").wait_recv()
        wi_out[:, local] += WZR[:, local].astype(F32)
    for n in range(3, 6):
        small_wait(n)
    small_out[...] = (SV[3] + AR[3]) + (AR[4] + AR[5])
    stores = [pltpu.make_async_copy(wi_out, wi_hbm, out_sem.at[PIECES])]
    row = 0
    for n, ref in enumerate((gain_hbm, bias_hbm, b_in_hbm, b_out_hbm)):
        piece = small_out.at[pl.ds(row, ref.shape[0])]
        stores.append(pltpu.make_async_copy(piece, ref, out_sem.at[PIECES + 1 + n]))
        row += ref.shape[0]
    for copy in stores:
        copy.start()
    for copy in started:
        copy.wait_send()

    @pl.when(inner)
    def _():
        for copy in (cut_own, cut_pair, back_near, back_far):
            copy.wait_send()

    for n in range(2):
        piece = W.at[1, wo_piece(img, n)]
        remote(piece, piece, yn, f"WY{n}").wait_send()
    for t in range(stride):
        ht_copy(t).wait_send()
    for copy in (wi_copy, *wo_copies, wg_copy(0, 1 - img), wg_copy(1, img)):
        copy.wait_send()

    @pl.loop(0, PIECES)
    def _(k):
        for copy in (x_copy, z_copy, d_copy, y_copy, zk_copy):
            copy(k).wait_send()

    @pl.loop(0, PIECES)
    def _(k):
        wo_store(k).wait()

    for copy in stores:
        copy.wait()


def finish_body(ins, outs, held, sems):
    pieces = []
    for source, place, target in zip(ins, held, outs):
        lines = source.shape[0]
        step = lines // 4 if lines >= 128 else lines
        for low in range(0, lines, step):
            rows = pl.ds(low, step)
            pieces.append((source.at[rows], place.at[rows], target.at[rows]))
    copies = []
    for n, (source, place, _) in enumerate(pieces):
        copies.append(pltpu.make_async_copy(source, place, sems.at[0, n]))
        copies[-1].start()
    later = []
    for n, (_, place, target) in enumerate(pieces):
        copies[n].wait()
        later.append(pltpu.make_async_copy(place, target, sems.at[1, n]))
        later[-1].start()
    for copy in later:
        copy.wait()


def finish(values):
    count = len(values)
    hbm = pl.BlockSpec(memory_space=pl.ANY)

    def body(*refs):
        finish_body(refs[:count], refs[count : 2 * count], refs[2 * count : -1], refs[-1])

    return pl.pallas_call(
        body,
        out_shape=[jax.ShapeDtypeStruct(v.shape, v.dtype) for v in values],
        in_specs=[hbm] * count,
        out_specs=[hbm] * count,
        scratch_shapes=[pltpu.VMEM(v.shape, v.dtype) for v in values]
        + [pltpu.SemaphoreType.DMA((2, 4 * count))],
    )(*values)


def per_device_kernel(
    vision_feats, ln_gain, ln_bias, w_in, b_in, w_out, lm_grad, image_counts, token_pos
):
    seq_count = lax.axis_size("seq")
    _, rows, half = lm_grad.shape
    hb = w_out.shape[0]
    dv = ln_gain.shape[0]
    frows = vision_feats.shape[1]
    tokens = token_pos.shape[1]
    samples = image_counts.shape[1]
    stride = seq_count // samples
    span = stride * rows
    part = span // 2
    hid = samples * hb
    images = tokens // PATCH
    lanes = 128
    small = (2 * dv + seq_count * hb + 2 * half) // lanes
    dims = (rows, half, hb, dv, frows, tokens, seq_count, samples, images)
    vmem = pl.BlockSpec(memory_space=pltpu.VMEM)
    smem = pl.BlockSpec(memory_space=pltpu.SMEM)
    hbm = pl.BlockSpec(memory_space=pl.ANY)
    wo, wi, *sums = pl.pallas_call(
        functools.partial(kernel_body, dims),
        out_shape=(
            jax.ShapeDtypeStruct((hb // 2, half), F32),
            jax.ShapeDtypeStruct((dv // 4, hb), F32),
            jax.ShapeDtypeStruct((dv // lanes, lanes), F32),
            jax.ShapeDtypeStruct((dv // lanes, lanes), F32),
            jax.ShapeDtypeStruct((seq_count * hb // lanes, lanes), F32),
            jax.ShapeDtypeStruct((2 * half // lanes, lanes), F32),
        ),
        in_specs=[smem, smem, hbm, vmem, vmem, hbm, vmem, hbm, hbm],
        out_specs=[hbm] * 6,
        scratch_shapes=[
            pltpu.VMEM((span, half), BF16),
            pltpu.VMEM((samples, hb, half), BF16),
            pltpu.VMEM((samples, dv, hb), BF16),
            pltpu.VMEM((tokens, dv), BF16),
            pltpu.VMEM((dv, part), BF16),
            pltpu.VMEM((part, dv), BF16),
            pltpu.VMEM((part, 1), F32),
            pltpu.VMEM((part, 1), F32),
            pltpu.VMEM((part, hid), F32),
            pltpu.VMEM((hid, span), BF16),
            pltpu.VMEM((stride, rows, hid), F32),
            pltpu.VMEM((part, hid), BF16),
            pltpu.VMEM((part, hid), BF16),
            pltpu.VMEM((hb, half), BF16),
            pltpu.VMEM((hb, half), BF16),
            pltpu.VMEM((hb // 2, half), BF16),
            pltpu.VMEM((hb // 2, half), BF16),
            pltpu.VMEM((hb // 2, half), F32),
            pltpu.VMEM((2, dv // 4, hid), BF16),
            pltpu.VMEM((2, dv // 4, hid), BF16),
            pltpu.VMEM((dv // 4, hid), BF16),
            pltpu.VMEM((dv // 4, hid), BF16),
            pltpu.VMEM((dv // 4, hb), BF16),
            pltpu.VMEM((dv // 4, hb), BF16),
            pltpu.VMEM((1, hb), F32),
            pltpu.VMEM((8, max(hid, dv)), F32),
            pltpu.VMEM((4, small, lanes), F32),
            pltpu.VMEM((6, small, lanes), F32),
            pltpu.VMEM((hb // 2, half), F32),
            pltpu.VMEM((dv // 4, hb), F32),
            pltpu.VMEM((small, lanes), F32),
            pltpu.SemaphoreType.DMA((PIECES + 5,)),
            pltpu.SemaphoreType.DMA((96,)),
            pltpu.SemaphoreType.DMA((96,)),
            pltpu.SemaphoreType.DMA((4,)),
        ],
        compiler_params=pltpu.CompilerParams(
            collective_id=0, has_side_effects=True, vmem_limit_bytes=67043328
        ),
    )(
        image_counts,
        token_pos,
        vision_feats[0],
        ln_gain[None],
        ln_bias[None],
        w_in,
        b_in[None],
        w_out,
        lm_grad[0],
    )
    wo, wi, *sums = finish((wo, wi, *sums))
    gain_grad, bias_grad, b_in_grad, b_out_grad = (value.reshape(-1) for value in sums)
    return (wi, b_in_grad, wo, b_out_grad, gain_grad, bias_grad)


def dispatch(mesh, *args):
    sizes = (mesh.shape["seq"], mesh.shape["img"], mesh.shape["fsdp"])
    if sizes == (8, 2, 2) and args[7].shape[1] == 2:
        return per_device_kernel(*args)
    return per_device(*args)


def solution(mesh):
    return jax.shard_map(
        functools.partial(dispatch, mesh),
        mesh=mesh,
        in_specs=(
            P("img", ("seq", "fsdp"), None),
            P(),
            P(),
            P("fsdp", "seq"),
            P("seq"),
            P("seq", "fsdp"),
            P("img", "seq", "fsdp"),
            P("img", None),
            P("img", None),
        ),
        out_specs=(
            P(("img", "fsdp"), "seq"),
            P(),
            P(("seq", "img"), "fsdp"),
            P(),
            P(),
            P(),
        ),
        check_vma=False,
    )
```
